128 devices in a mesh: row: 8 (over y, x_hi), col: 16 (over z, x_lo, core).
Axes of the slice: x: 4 (x_hi: 2, x_lo: 2; x = x_hi * 2 + x_lo), y: 4, z: 4, core: 2. Of those that a mesh axis runs over, the one named last changes fastest.
Arguments:
- h_slab: bfloat16 [4096, 96000], P('row', 'col'), may hold values from -0.01953125 to 0.01953125
- vectors: bfloat16 [96000, 1024], P('col'), may hold values from -6 to 6
- left_rows: bfloat16 [4096, 1024], P('row'), may hold values from -0.09375 to 0.09375
Outputs:
- projected: float32 [1024, 1024], replicated
The draws below stay inside these ranges and needn't reach their ends.
All inputs are finite; a program needn't handle non-finite values.
Results may differ from the reference program's by a relative error of at most 0.0003.
Values sent between devices are 32-bit elements; how exact they have to be, the bound alone decides.
No kernel may reach another device: no remote copies, remote signals or barrier semaphores. Data moves between devices by JAX's collectives and lax.ppermute only.
A program may use at most 128 MiB of HBM per device.

```python
import jax
import jax.numpy as jnp
from jax import lax

ORDER = 96000
NVEC = 1024
SLAB_ROWS = 4096


def block_levels(rng, dims, split, smallest, high):
    def one(position, parts):
        steps = jax.random.uniform(jax.random.fold_in(jax.random.fold_in(rng, 6), position), (parts,), jnp.float32, smallest / len(split), high / len(split))
        return jnp.repeat(jnp.exp(steps), dims[position] // parts).reshape((-1,) + (1,) * (len(dims) - position - 1))

    level = one(*split[0])
    for cut in split[1:]:
        level = level * one(*cut)
    return level


def bell_draw(stream_key, shape, deviation, most, shards=(), kind=jnp.bfloat16):
    result = jax.random.normal(stream_key, shape, jnp.float32) * deviation
    if len(shards) > 0:
        result = block_levels(stream_key, shape, shards, -0.22, 0.18) * result
    return jnp.clip(result, min=-most, max=most).astype(kind)


def setup_inputs(seed: int = 0) -> dict:
    splits = jax.random.split(jax.random.key(seed), 4)
    return {
        "h_slab": bell_draw(splits[0], (SLAB_ROWS, ORDER), ORDER ** -0.5, 0.01953125, ((0, 8), (1, 16))),
        "vectors": bell_draw(splits[1], (ORDER, NVEC), 1.0, 6.0, ((0, 16),)),
        "left_rows": bell_draw(splits[2], (SLAB_ROWS, NVEC), SLAB_ROWS ** -0.5, 0.09375, ((0, 8),)),
    }


def reference(h_slab, vectors, left_rows):
    product = jnp.dot(h_slab, vectors, preferred_element_type=jnp.float32)
    left_wide = left_rows.astype(jnp.float32)
    projected = jnp.dot(left_wide.T, product, precision=lax.Precision.HIGHEST)
    return projected
```

```python
import jax
import jax.numpy as jnp
from jax import lax
from jax.sharding import Mesh, PartitionSpec as P


PLANE = ("y", "xh", "xl")


def shift(value, axis, step):
    size = lax.axis_size(axis)
    return lax.ppermute(value, axis, [(i, (i + step) % size) for i in range(size)])


def pick(parts, index):
    return lax.dynamic_index_in_dim(parts, index % parts.shape[0], 0, keepdims=False)


def reduce_ring(parts):
    me = lax.axis_index("z")
    half = parts.shape[1] // 2
    far = pick(parts, me + 2)
    from_below = shift(far[:half], "z", 1)
    from_above = shift(far[half:], "z", -1)
    above, below = pick(parts, me + 1), pick(parts, me + 3)
    above = jnp.concatenate([above[:half] + from_below, above[half:]])
    below = jnp.concatenate([below[:half], below[half:] + from_above])
    return pick(parts, me) + shift(above, "z", 1) + shift(below, "z", -1)


def body(h_slab, vectors, left_rows):
    core = lax.axis_index("core")
    me = lax.axis_index("z")
    product = lax.dot_general(
        vectors, h_slab, (((0,), (1,)), ((), ())), preferred_element_type=jnp.float32
    )
    nvec, rows = product.shape
    halves = product.reshape(2, nvec // 2, rows)
    mine = pick(halves, core) + shift(pick(halves, core + 1), "core", 1)
    shared = reduce_ring(mine.reshape(4, nvec // 8, rows))
    local_part = lax.dot_general(
        left_rows.astype(jnp.float32),
        shared,
        (((0,), (1,)), ((), ())),
        precision=lax.Precision.HIGHEST,
        preferred_element_type=jnp.float32,
    )
    parts = local_part.reshape(16, nvec // 16, nvec // 8)
    parts = lax.all_to_all(parts, PLANE, 0, 0, tiled=True)
    summed = jnp.sum(parts, axis=0)
    copies = jnp.broadcast_to(summed, (16, *summed.shape))
    block = lax.all_to_all(copies, PLANE, 0, 0, tiled=True).reshape(nvec, nvec // 8)

    half = nvec // 2
    below = shift(block, "z", 1)
    above = shift(block, "z", -1)
    other = shift(block, "core", 1)
    far_low = shift(below[:half], "z", 1)
    far_high = shift(above[half:], "z", -1)
    other_near = shift(jnp.stack([above, below]), "core", 1)
    far = jnp.concatenate([far_low, far_high])
    other_far = shift(far, "core", 1)
    mine4 = jnp.stack([block, above, far, below])
    other4 = jnp.stack([other, other_near[0], other_far, other_near[1]])
    order = (jnp.arange(4) - me) % 4
    mine4 = jnp.take(mine4, order, axis=0)
    other4 = jnp.take(other4, order, axis=0)
    low = jnp.where(core == 0, mine4, other4)
    high = jnp.where(core == 0, other4, mine4)
    whole = jnp.concatenate([low, high])
    return jnp.moveaxis(whole, 0, 1).reshape(nvec, nvec)


def solution(mesh):
    fine = Mesh(mesh.devices.reshape(4, 2, 4, 2, 2), ("y", "xh", "z", "xl", "core"))
    row, col = ("y", "xh"), ("z", "xl", "core")
    in_specs = (P(row, col), P(col, None), P(row, None))
    return jax.shard_map(body, mesh=fine, in_specs=in_specs, out_specs=P(), check_vma=False)
```

```python
import functools

import jax
import jax.numpy as jnp
from jax import lax
from jax.experimental import pallas as pl
from jax.experimental.pallas import tpu as pltpu
from jax.sharding import Mesh, PartitionSpec as P


AXES = ("y", "xh", "z", "xl", "core")
SIZES = (4, 2, 4, 2, 2)
PLANE = ("y", "xh", "xl")


def rank(y, x, z, core):
    return (((y * 2 + x // 2) * 4 + z) * 2 + x % 2) * 2 + core


def shift(value, axis, step):
    size = lax.axis_size(axis)
    return lax.ppermute(value, axis, [(i, (i + step) % size) for i in range(size)])


def ring_shift(value, step):
    pairs = []
    for y in range(4):
        for x in range(4):
            for z in range(4):
                pairs.append((rank(y, x, z, 0), rank(y, x, (z + step) % 4, 0)))
                pairs.append((rank(y, x, z, 1), rank((y + step) % 4, x, z, 1)))
    return lax.ppermute(value, AXES, pairs)


def plane_groups():
    groups = [[rank(y, x, z, 0) for y in range(4) for x in range(4)] for z in range(4)]
    return groups + [[rank(y, x, z, 1) for z in range(4) for x in range(4)] for y in range(4)]


def pick(parts, index):
    return lax.dynamic_index_in_dim(parts, index % parts.shape[0], 0, keepdims=False)


def reduce_ring(parts):
    me = lax.axis_index("z")
    half = parts.shape[1] // 2
    far = pick(parts, me + 2)
    from_below = shift(far[:half], "z", 1)
    from_above = shift(far[half:], "z", -1)
    above, below = pick(parts, me + 1), pick(parts, me + 3)
    above = jnp.concatenate([above[:half] + from_below, above[half:]])
    below = jnp.concatenate([below[:half], below[half:] + from_above])
    return pick(parts, me) + shift(above, "z", 1) + shift(below, "z", -1)


def place_kernel(where, *refs):
    own, other, out, sem = refs[:7], refs[7:14], refs[14], refs[15]
    y, z, core = where[0], where[1], where[2]

    def pieces(blocks):
        block, below_low, below_high, above_low, above_high, far_low, far_high = blocks
        half = below_low.shape[0]
        yield block.at[pl.ds(0, half)], 0, 0
        yield block.at[pl.ds(half, half)], 0, 1
        yield above_low, 1, 0
        yield above_high, 1, 1
        yield far_low, 2, 0
        yield far_high, 2, 1
        yield below_low, 3, 0
        yield below_high, 3, 1

    def copies(first, second):
        made = []
        for ref, ahead, part in pieces(first):
            column = pl.multiple_of(lax.rem(z + ahead, 4) * 128, 128)
            made.append((ref, out.at[pl.ds(part * 512, 512), pl.ds(column, 128)]))
        for ref, ahead, part in pieces(second):
            row = pl.multiple_of(lax.rem(y + ahead, 4) * 256, 256)
            for k in range(2):
                place = out.at[pl.ds(row, 256), pl.ds(512 + (part * 2 + k) * 128, 128)]
                made.append((ref.at[pl.ds(k * 256, 256)], place))
        return [pltpu.make_async_copy(src, dst, sem.at[i]) for i, (src, dst) in enumerate(made)]

    def run(first, second):
        made = copies(first, second)
        for copy in made:
            copy.start()
        for copy in made:
            copy.wait()

    @pl.when(core == 0)
    def _():
        run(own, other)

    @pl.when(core == 1)
    def _():
        run(other, own)


def place(where, own, other, nvec):
    return pl.pallas_call(
        place_kernel,
        out_shape=jax.ShapeDtypeStruct((nvec, nvec), jnp.float32),
        in_specs=[pl.BlockSpec(memory_space=pltpu.SMEM)] + [pl.BlockSpec(memory_space=pltpu.VMEM)] * 14,
        out_specs=pl.BlockSpec(memory_space=pl.ANY),
        scratch_shapes=[pltpu.SemaphoreType.DMA((24,))],
        name="place",
    )(where, *own, *other)


def body(h_slab, vectors, left_rows):
    y, z, core = lax.axis_index("y"), lax.axis_index("z"), lax.axis_index("core")
    product = lax.dot_general(
        vectors, h_slab, (((0,), (1,)), ((), ())), preferred_element_type=jnp.float32
    )
    nvec, rows = product.shape
    halves = product.reshape(2, nvec // 2, rows)
    mine = pick(halves, core) + shift(pick(halves, core + 1), "core", 1)
    shared = reduce_ring(mine.reshape(4, nvec // 8, rows))
    local_part = lax.dot_general(
        left_rows.astype(jnp.float32),
        shared,
        (((0,), (1,)), ((), ())),
        precision=lax.Precision.HIGHEST,
        preferred_element_type=jnp.float32,
    )
    parts = local_part.reshape(16, nvec // 16, nvec // 8)
    parts = lax.all_to_all(parts, PLANE, 0, 0, tiled=True)
    summed = jnp.sum(parts, axis=0)
    copies = jnp.broadcast_to(summed, (16, *summed.shape))
    block = lax.all_to_all(
        copies, AXES, 0, 0, tiled=True, axis_index_groups=plane_groups()
    ).reshape(nvec, nvec // 8)

    half = nvec // 2
    low, high = block[:half], block[half:]
    below_low = ring_shift(low, 1)
    above_high = ring_shift(high, -1)
    below_high = ring_shift(high, 1)
    above_low = ring_shift(low, -1)
    far_low = ring_shift(below_low, 1)
    far_high = ring_shift(above_high, -1)
    own = [block, below_low, below_high, above_low, above_high, far_low, far_high]
    other = [shift(value, "core", 1) for value in own]
    return place(jnp.stack([y, z, core]), own, other, nvec)


def solution(mesh):
    fine = Mesh(mesh.devices.reshape(SIZES), AXES)
    row, col = ("y", "xh"), ("z", "xl", "core")
    in_specs = (P(row, col), P(col, None), P(row, None))
    return jax.shard_map(body, mesh=fine, in_specs=in_specs, out_specs=P(), check_vma=False)
```

```python
import jax
import jax.numpy as jnp
from jax import lax
from jax.experimental import pallas as pl
from jax.experimental.pallas import tpu as pltpu
from jax.sharding import Mesh, PartitionSpec as P


AXES = ("y", "xh", "z", "xl", "core")
SIZES = (4, 2, 4, 2, 2)
PLANE = ("y", "xh", "xl")
F32 = jnp.float32
ANY = pl.BlockSpec(memory_space=pl.ANY)
HBM = pl.BlockSpec(memory_space=pltpu.HBM)
VMEM = pl.BlockSpec(memory_space=pltpu.VMEM)


def rank(y, x, z, core):
    return (((y * 2 + x // 2) * 4 + z) * 2 + x % 2) * 2 + core


def shift(value, axis, step):
    size = lax.axis_size(axis)
    return lax.ppermute(value, axis, [(i, (i + step) % size) for i in range(size)])


def ring_shift(value, step):
    pairs = []
    for y in range(4):
        for x in range(4):
            for z in range(4):
                pairs.append((rank(y, x, z, 0), rank(y, x, (z + step) % 4, 0)))
                pairs.append((rank(y, x, z, 1), rank((y + step) % 4, x, z, 1)))
    return lax.ppermute(value, AXES, pairs)


def plane_groups():
    groups = [[rank(y, x, z, 0) for y in range(4) for x in range(4)] for z in range(4)]
    return groups + [[rank(y, x, z, 1) for z in range(4) for x in range(4)] for y in range(4)]


def resident(value):
    return pltpu.with_memory_space_constraint(value, pltpu.VMEM)


def streamed(value):
    return pltpu.with_memory_space_constraint(value, pltpu.HBM)


def cuts(depth, step):
    return [(start, min(step, depth - start)) for start in range(0, depth, step)]


def emit(total, part, keep, give):
    core = lax.axis_index("core")
    rows = total.shape[0] // 4
    for k in range(2):
        base = lax.rem(part + k, 2) * (2 * rows)
        mine = pl.multiple_of(base + core * rows, rows)
        theirs = pl.multiple_of(base + (1 - core) * rows, rows)
        keep[pl.ds(k * rows, rows), :] = total[pl.ds(mine, rows), :]
        give[pl.ds(k * rows, rows), :] = total[pl.ds(theirs, rows), :]


def multiply(left, right):
    return lax.dot_general(left, right, (((0,), (0,)), ((), ())), preferred_element_type=F32)


def first_kernel(h, v, keep, give, h_here, v_here, total, sem):
    z = lax.axis_index("z")
    width = v_here.shape[1]
    column = pl.multiple_of((1 - z // 2) * width, width)
    copies = []
    for i, (start, size) in enumerate(cuts(h.shape[0], 2048)):
        rows = pl.ds(start, size)
        one = pltpu.make_async_copy(h.at[rows], h_here.at[rows], sem.at[2 * i])
        two = pltpu.make_async_copy(v.at[rows, pl.ds(column, width)], v_here.at[rows], sem.at[2 * i + 1])
        one.start()
        two.start()
        copies.append((start, size, one, two))
    for start, size, one, two in copies:
        one.wait()
        two.wait()
        part = multiply(v_here[start : start + size], h_here[start : start + size])
        if start == 0:
            total[...] = part
        else:
            total[...] += part
    emit(total, lax.rem(z, 2), keep, give)


def second_kernel(h_here, v, keep, give, v_here, total, sem):
    z = lax.axis_index("z")
    width = v_here.shape[1]
    column = pl.multiple_of((z // 2) * width, width)
    copies = []
    for i, (start, size) in enumerate(cuts(h_here.shape[0], 1536)):
        rows = pl.ds(start, size)
        copy = pltpu.make_async_copy(v.at[rows, pl.ds(column, width)], v_here.at[rows], sem.at[i])
        copy.start()
        copies.append((start, size, copy))
    for start, size, copy in copies:
        copy.wait()
        part = multiply(v_here[start : start + size], h_here[start : start + size])
        if start == 0:
            total[...] = part
        else:
            total[...] += part
    emit(total, lax.rem(z, 2), keep, give)


def first_half(h, v):
    depth, rows = h.shape
    width = v.shape[1] // 2
    piece = pltpu.VMEM((width // 2, rows), F32)
    return pl.pallas_call(
        first_kernel,
        in_specs=[HBM, HBM],
        out_specs=[VMEM] * 3,
        out_shape=[piece, piece, pltpu.VMEM((depth, rows), h.dtype)],
        scratch_shapes=[
            pltpu.VMEM((depth, width), v.dtype),
            pltpu.VMEM((width, rows), F32),
            pltpu.SemaphoreType.DMA((2 * len(cuts(depth, 2048)),)),
        ],
        compiler_params=pltpu.CompilerParams(vmem_limit_bytes=40 * 2**20),
        name="first_half",
    )(streamed(h), streamed(v))


def second_half(h_here, v):
    depth, rows = h_here.shape
    width = v.shape[1] // 2
    piece = pltpu.VMEM((width // 2, rows), F32)
    return pl.pallas_call(
        second_kernel,
        in_specs=[VMEM, HBM],
        out_specs=[VMEM] * 2,
        out_shape=[piece, piece],
        scratch_shapes=[
            pltpu.VMEM((depth, width), v.dtype),
            pltpu.VMEM((width, rows), F32),
            pltpu.SemaphoreType.DMA((len(cuts(depth, 1536)),)),
        ],
        compiler_params=pltpu.CompilerParams(vmem_limit_bytes=40 * 2**20),
        name="second_half",
    )(resident(h_here), streamed(v))


def near_kernel(*refs):
    own, other, out, sem = refs[:3], refs[3:6], refs[6], refs[7]
    steps = (0, 3, 1)
    write([(ref, step, 0) for ref, step in zip(own, steps)], [(ref, step, 0) for ref, step in zip(other, steps)], out, sem)


def far_kernel(*refs):
    own, other, out, sem = refs[:2], refs[2:4], refs[5], refs[6]
    write([(own[0], 2, 0), (own[1], 2, 1)], [(other[0], 2, 0), (other[1], 2, 1)], out, sem)


def write(own, other, out, sem):
    y, z, core = lax.axis_index("y"), lax.axis_index("z"), lax.axis_index("core")

    def run(first, second):
        made = []
        for ref, step, part in first:
            rows = ref.shape[0]
            column = pl.multiple_of(lax.rem(z + step, 4) * 256, 256)
            made.append((ref, out.at[pl.ds(part * rows, rows), pl.ds(column, 128)]))
        for ref, step, part in second:
            row = pl.multiple_of(lax.rem(y + step, 4) * 256, 256)
            for k in range(ref.shape[0] // 256):
                column = (part * 2 + k) * 256 + 128
                made.append((ref.at[pl.ds(k * 256, 256)], out.at[pl.ds(row, 256), pl.ds(column, 128)]))
        made = [pltpu.make_async_copy(src, dst, sem.at[i]) for i, (src, dst) in enumerate(made)]
        for copy in made:
            copy.start()
        for copy in made:
            copy.wait()

    @pl.when(core == 0)
    def _():
        run(own, other)

    @pl.when(core == 1)
    def _():
        run(other, own)


def place_near(own, other, nvec):
    return pl.pallas_call(
        near_kernel,
        in_specs=[ANY] * 6,
        out_specs=ANY,
        out_shape=jax.ShapeDtypeStruct((nvec, nvec), F32),
        scratch_shapes=[pltpu.SemaphoreType.DMA((15,))],
        compiler_params=pltpu.CompilerParams(vmem_limit_bytes=2**20),
        name="place_near",
    )(*own, *other)


def place_far(own, other, whole):
    return pl.pallas_call(
        far_kernel,
        in_specs=[ANY] * 5,
        out_specs=ANY,
        out_shape=jax.ShapeDtypeStruct(whole.shape, F32),
        input_output_aliases={4: 0},
        scratch_shapes=[pltpu.SemaphoreType.DMA((6,))],
        compiler_params=pltpu.CompilerParams(vmem_limit_bytes=2**20),
        name="place_far",
    )(*own, *other, whole)


def body(h_slab, vectors, left_rows):
    z = lax.axis_index("z")
    nvec = vectors.shape[1]
    wide = nvec // 8
    keep, give, h_here = first_half(h_slab.T, vectors)
    sums = keep + shift(give, "core", 1)
    far, mate = sums[:wide], sums[wide:]
    keep, give = second_half(h_here, vectors)
    from_below = shift(far[: wide // 2], "z", 1)
    from_above = shift(far[wide // 2 :], "z", -1)
    sums = keep + shift(give, "core", 1)
    own, twin = sums[:wide], sums[wide:]
    even = z % 2 == 0
    above, below = jnp.where(even, twin, mate), jnp.where(even, mate, twin)
    above = jnp.concatenate([above[: wide // 2] + from_below, above[wide // 2 :]])
    below = jnp.concatenate([below[: wide // 2], below[wide // 2 :] + from_above])
    shared = own + shift(above, "z", 1) + shift(below, "z", -1)

    local_part = lax.dot_general(
        left_rows.astype(F32),
        shared,
        (((0,), (1,)), ((), ())),
        precision=lax.Precision.HIGHEST,
        preferred_element_type=F32,
    )
    parts = local_part.reshape(16, nvec // 16, wide)
    parts = lax.all_to_all(parts, PLANE, 0, 0, tiled=True)
    summed = jnp.sum(parts, axis=0)
    copies = jnp.broadcast_to(summed, (16, *summed.shape))
    block = lax.all_to_all(
        copies, AXES, 0, 0, tiled=True, axis_index_groups=plane_groups()
    ).reshape(nvec, wide)

    half = nvec // 2
    below = ring_shift(block, 1)
    above = ring_shift(block, -1)
    far_low = ring_shift(below[:half], 1)
    far_high = ring_shift(above[half:], -1)
    near = [block, below, above]
    far = [far_low, far_high]
    whole = place_near(near, [shift(value, "core", 1) for value in near], nvec)
    return place_far(far, [shift(value, "core", 1) for value in far], whole)


def solution(mesh):
    fine = Mesh(mesh.devices.reshape(SIZES), AXES)
    row, col = ("y", "xh"), ("z", "xl", "core")
    in_specs = (P(row, col), P(col, None), P(row, None))
    return jax.shard_map(body, mesh=fine, in_specs=in_specs, out_specs=P(), check_vma=False)
```

```python
import functools

import jax
import jax.numpy as jnp
from jax import lax
from jax.experimental import pallas as pl
from jax.experimental.pallas import tpu as pltpu
from jax.sharding import Mesh, PartitionSpec as P


AXES = ("y", "xh", "z", "xl", "core")
SIZES = (4, 2, 4, 2, 2)
PLANE = ("y", "xh", "xl")
F32 = jnp.float32
ANY = pl.BlockSpec(memory_space=pl.ANY)
HBM = pl.BlockSpec(memory_space=pltpu.HBM)
VMEM = pl.BlockSpec(memory_space=pltpu.VMEM)


def rank(y, x, z, core):
    return (((y * 2 + x // 2) * 4 + z) * 2 + x % 2) * 2 + core


def shift(value, axis, step):
    size = lax.axis_size(axis)
    return lax.ppermute(value, axis, [(i, (i + step) % size) for i in range(size)])


def ring_shift(value, step):
    pairs = []
    for y in range(4):
        for x in range(4):
            for z in range(4):
                pairs.append((rank(y, x, z, 0), rank(y, x, (z + step) % 4, 0)))
                pairs.append((rank(y, x, z, 1), rank((y + step) % 4, x, z, 1)))
    return lax.ppermute(value, AXES, pairs)


def plane_groups():
    groups = [[rank(y, x, z, 0) for y in range(4) for x in range(4)] for z in range(4)]
    return groups + [[rank(y, x, z, 1) for z in range(4) for x in range(4)] for y in range(4)]


def resident(value):
    return pltpu.with_memory_space_constraint(value, pltpu.VMEM)


def streamed(value):
    return pltpu.with_memory_space_constraint(value, pltpu.HBM)


def cuts(depth):
    return [(start, min(1536, depth - start)) for start in range(0, depth, 1536)]


def multiply(left, right):
    return lax.dot_general(left, right, (((0,), (0,)), ((), ())), preferred_element_type=F32)


def columns_of(v, ahead, rows=None):
    width = v.shape[1] // 4
    column = pl.multiple_of(lax.rem(lax.axis_index("z") + ahead, 4) * width, width)
    return v.at[:, pl.ds(column, width)] if rows is None else v.at[rows, pl.ds(column, width)]


def emit(total, keep, give):
    core = lax.axis_index("core")
    rows = total.shape[0] // 2
    keep[...] = total[pl.ds(pl.multiple_of(core * rows, rows), rows), :]
    give[...] = total[pl.ds(pl.multiple_of((1 - core) * rows, rows), rows), :]


def opening_kernel(ahead, following, h, v, keep, give, h_here, v_next, v_here, total, sem):
    copies = []
    for i, (start, size) in enumerate(cuts(h.shape[0])):
        rows = pl.ds(start, size)
        one = pltpu.make_async_copy(h.at[rows], h_here.at[rows], sem.at[2 * i])
        two = pltpu.make_async_copy(columns_of(v, ahead, rows), v_here.at[rows], sem.at[2 * i + 1])
        one.start()
        two.start()
        copies.append((start, size, one, two))
    fetch = pltpu.make_async_copy(columns_of(v, following), v_next, sem.at[2 * len(copies)])
    fetch.start()
    for start, size, one, two in copies:
        one.wait()
        two.wait()
        part = multiply(v_here[start : start + size], h_here[start : start + size])
        if start == 0:
            total[...] = part
        else:
            total[...] += part
    emit(total, keep, give)
    fetch.wait()


def middle_kernel(following, h_here, v_here, v, keep, give, v_next, total, sem):
    fetch = pltpu.make_async_copy(columns_of(v, following), v_next, sem)
    fetch.start()
    total[...] = multiply(v_here[...], h_here[...])
    emit(total, keep, give)
    fetch.wait()


def closing_kernel(h_here, v_here, keep, give, total):
    total[...] = multiply(v_here[...], h_here[...])
    emit(total, keep, give)


def kernel_call(kernel, h, v, ins, outs, scratch):
    width, rows = v.shape[1] // 4, h.shape[1]
    piece = pltpu.VMEM((width // 2, rows), F32)
    return pl.pallas_call(
        kernel,
        in_specs=ins,
        out_specs=[VMEM] * (2 + len(outs)),
        out_shape=[piece, piece, *outs],
        scratch_shapes=scratch,
        cost_estimate=pl.CostEstimate(flops=2 * h.shape[0] * width * rows, bytes_accessed=h.shape[0] * width * 2, transcendentals=0),
        compiler_params=pltpu.CompilerParams(vmem_limit_bytes=8 * 2**20),
    )


def products(h, v):
    depth, rows = h.shape
    block = pltpu.VMEM((depth, v.shape[1] // 4), v.dtype)
    slab = pltpu.VMEM((depth, rows), h.dtype)
    total = pltpu.VMEM((v.shape[1] // 4, rows), F32)
    v = streamed(v)
    sems = pltpu.SemaphoreType.DMA((2 * len(cuts(depth)) + 1,))

    def opening(ahead, following):
        kernel = functools.partial(opening_kernel, ahead, following)
        return kernel_call(kernel, h, v, [HBM, HBM], [slab, block], [block, total, sems])(streamed(h), v)

    def middle(following, h_here, v_here):
        kernel = functools.partial(middle_kernel, following)
        call = kernel_call(kernel, h, v, [VMEM, VMEM, HBM], [block], [total, pltpu.SemaphoreType.DMA])
        return call(resident(h_here), resident(v_here), v)

    def closing(h_here, v_here):
        call = kernel_call(closing_kernel, h, v, [VMEM, VMEM], [], [total])
        return call(resident(h_here), resident(v_here))

    return opening, middle, closing


def near_kernel(*refs):
    own, other, out, sem = refs[:3], refs[3:6], refs[6], refs[7]
    steps = (0, 3, 1)
    write([(ref, step, 0) for ref, step in zip(own, steps)], [(ref, step, 0) for ref, step in zip(other, steps)], out, sem)


def far_kernel(*refs):
    own, other, out, sem = refs[:2], refs[2:4], refs[5], refs[6]
    write([(own[0], 2, 0), (own[1], 2, 1)], [(other[0], 2, 0), (other[1], 2, 1)], out, sem)


def write(own, other, out, sem):
    y, z, core = lax.axis_index("y"), lax.axis_index("z"), lax.axis_index("core")

    def run(first, second):
        made = []
        for ref, step, part in first:
            rows = ref.shape[0]
            column = pl.multiple_of(lax.rem(z + step, 4) * 256, 256)
            made.append((ref, out.at[pl.ds(part * rows, rows), pl.ds(column, 128)]))
        for ref, step, part in second:
            row = pl.multiple_of(lax.rem(y + step, 4) * 256, 256)
            for k in range(ref.shape[0] // 256):
                column = (part * 2 + k) * 256 + 128
                made.append((ref.at[pl.ds(k * 256, 256)], out.at[pl.ds(row, 256), pl.ds(column, 128)]))
        made = [pltpu.make_async_copy(src, dst, sem.at[i]) for i, (src, dst) in enumerate(made)]
        for copy in made:
            copy.start()
        for copy in made:
            copy.wait()

    @pl.when(core == 0)
    def _():
        run(own, other)

    @pl.when(core == 1)
    def _():
        run(other, own)


def place_near(own, other, nvec):
    return pl.pallas_call(
        near_kernel,
        in_specs=[ANY] * 6,
        out_specs=ANY,
        out_shape=jax.ShapeDtypeStruct((nvec, nvec), F32),
        scratch_shapes=[pltpu.SemaphoreType.DMA((15,))],
        compiler_params=pltpu.CompilerParams(vmem_limit_bytes=2**20),
        name="place_near",
    )(*own, *other)


def place_far(own, other, whole):
    return pl.pallas_call(
        far_kernel,
        in_specs=[ANY] * 5,
        out_specs=ANY,
        out_shape=jax.ShapeDtypeStruct(whole.shape, F32),
        input_output_aliases={4: 0},
        scratch_shapes=[pltpu.SemaphoreType.DMA((6,))],
        compiler_params=pltpu.CompilerParams(vmem_limit_bytes=2**20),
        name="place_far",
    )(*own, *other, whole)


def body(h_slab, vectors, left_rows):
    nvec = vectors.shape[1]
    wide = nvec // 8
    half = wide // 2
    opening, middle, closing = products(h_slab.T, vectors)

    far, give, h_here, v_next = opening(2, 1)
    other_far = shift(give, "core", 1)
    up, give, v_next = middle(3, h_here, v_next)
    other_up = shift(give, "core", 1)
    far = far + other_far
    from_below = shift(far[:half], "z", 1)
    from_above = shift(far[half:], "z", -1)
    down, give, v_next = middle(0, h_here, v_next)
    other_down = shift(give, "core", 1)
    up, down = up + other_up, down + other_down
    up = jnp.concatenate([up[:half] + from_below, up[half:]])
    down = jnp.concatenate([down[:half], down[half:] + from_above])
    from_below = shift(up, "z", 1)
    from_above = shift(down, "z", -1)
    own, give = closing(h_here, v_next)
    shared = own + shift(give, "core", 1) + from_below + from_above

    local_part = lax.dot_general(
        left_rows.astype(F32),
        shared,
        (((0,), (1,)), ((), ())),
        precision=lax.Precision.HIGHEST,
        preferred_element_type=F32,
    )
    parts = local_part.reshape(16, nvec // 16, wide)
    parts = lax.all_to_all(parts, PLANE, 0, 0, tiled=True)
    summed = jnp.sum(parts, axis=0)
    copies = jnp.broadcast_to(summed, (16, *summed.shape))
    block = lax.all_to_all(
        copies, AXES, 0, 0, tiled=True, axis_index_groups=plane_groups()
    ).reshape(nvec, wide)

    half = nvec // 2
    below = ring_shift(block, 1)
    above = ring_shift(block, -1)
    other = shift(block, "core", 1)
    far_low = ring_shift(below[:half], 1)
    far_high = ring_shift(above[half:], -1)
    other_below = shift(below, "core", 1)
    other_above = shift(above, "core", 1)
    whole = place_near([block, below, above], [other, other_below, other_above], nvec)
    far = [far_low, far_high]
    return place_far(far, [shift(value, "core", 1) for value in far], whole)


def solution(mesh):
    fine = Mesh(mesh.devices.reshape(SIZES), AXES)
    row, col = ("y", "xh"), ("z", "xl", "core")
    in_specs = (P(row, col), P(col, None), P(row, None))
    return jax.shard_map(body, mesh=fine, in_specs=in_specs, out_specs=P(), check_vma=False)
```

```python
import functools

import jax
import jax.numpy as jnp
from jax import lax
from jax.experimental import pallas as pl
from jax.experimental.pallas import tpu as pltpu
from jax.sharding import Mesh, PartitionSpec as P


AXES = ("y", "xh", "z", "xl", "core")
SIZES = (4, 2, 4, 2, 2)
PLANE = ("y", "xh", "xl")
F32 = jnp.float32
ANY = pl.BlockSpec(memory_space=pl.ANY)
HBM = pl.BlockSpec(memory_space=pltpu.HBM)
VMEM = pl.BlockSpec(memory_space=pltpu.VMEM)


def rank(y, x, z, core):
    return (((y * 2 + x // 2) * 4 + z) * 2 + x % 2) * 2 + core


def shift(value, axis, step):
    size = lax.axis_size(axis)
    return lax.ppermute(value, axis, [(i, (i + step) % size) for i in range(size)])


def ring_shift(value, step):
    pairs = []
    for y in range(4):
        for x in range(4):
            for z in range(4):
                pairs.append((rank(y, x, z, 0), rank(y, x, (z + step) % 4, 0)))
                pairs.append((rank(y, x, z, 1), rank((y + step) % 4, x, z, 1)))
    return lax.ppermute(value, AXES, pairs)


def plane_groups():
    groups = [[rank(y, x, z, 0) for y in range(4) for x in range(4)] for z in range(4)]
    return groups + [[rank(y, x, z, 1) for z in range(4) for x in range(4)] for y in range(4)]


def resident(value):
    return pltpu.with_memory_space_constraint(value, pltpu.VMEM)


def streamed(value):
    return pltpu.with_memory_space_constraint(value, pltpu.HBM)


def cuts(depth):
    return [(start, min(1536, depth - start)) for start in range(0, depth, 1536)]


def multiply(left, right):
    return lax.dot_general(left, right, (((0,), (0,)), ((), ())), preferred_element_type=F32)


def columns_of(v, ahead, rows):
    width = v.shape[1] // 4
    column = pl.multiple_of(lax.rem(lax.axis_index("z") + ahead, 4) * width, width)
    return v.at[rows, pl.ds(column, width)]


def emit(total, keep, give):
    core = lax.axis_index("core")
    rows = total.shape[0] // 2
    keep[...] = total[pl.ds(pl.multiple_of(core * rows, rows), rows), :]
    give[...] = total[pl.ds(pl.multiple_of((1 - core) * rows, rows), rows), :]


def fetch(v, ahead, here, sem, base):
    copies = []
    for i, (start, size) in enumerate(cuts(v.shape[0])):
        rows = pl.ds(start, size)
        copies.append(pltpu.make_async_copy(columns_of(v, ahead, rows), here.at[rows], sem.at[base + i]))
    return copies


def accumulate(total, v_here, h_here, start, size):
    part = multiply(v_here[start : start + size], h_here[start : start + size])
    if start == 0:
        total[...] = part
    else:
        total[...] += part


def opening_kernel(ahead, h, v, keep, give, h_here, v_here, total, sem):
    spans = cuts(h.shape[0])
    ours = fetch(v, ahead, v_here, sem, 0)
    slab = []
    for i, (start, size) in enumerate(spans):
        rows = pl.ds(start, size)
        slab.append(pltpu.make_async_copy(h.at[rows], h_here.at[rows], sem.at[len(spans) + i]))
    for one, two in zip(slab, ours):
        one.start()
        two.start()
    for (start, size), one, two in zip(spans, slab, ours):
        one.wait()
        two.wait()
        accumulate(total, v_here, h_here, start, size)
    emit(total, keep, give)


def second_kernel(ahead, following, h_here, v, keep, give, v_next, v_here, total, sem):
    spans = cuts(v.shape[0])
    ours = fetch(v, ahead, v_here, sem, 0)
    theirs = fetch(v, following, v_next, sem, len(spans))
    for copy in (*ours, *theirs):
        copy.start()
    for (start, size), copy in zip(spans, ours):
        copy.wait()
        accumulate(total, v_here, h_here, start, size)
    emit(total, keep, give)
    for copy in theirs:
        copy.wait()


def third_kernel(following, h_here, v_here, v, keep, give, v_next, total, sem):
    theirs = fetch(v, following, v_next, sem, 0)
    for copy in theirs:
        copy.start()
    total[...] = multiply(v_here[...], h_here[...])
    emit(total, keep, give)
    for copy in theirs:
        copy.wait()


def closing_kernel(h_here, v_here, keep, give, total):
    total[...] = multiply(v_here[...], h_here[...])
    emit(total, keep, give)


def kernel_call(kernel, h, v, ins, outs, scratch):
    width, rows = v.shape[1] // 4, h.shape[1]
    piece = pltpu.VMEM((width // 2, rows), F32)
    return pl.pallas_call(
        kernel,
        in_specs=ins,
        out_specs=[VMEM] * (2 + len(outs)),
        out_shape=[piece, piece, *outs],
        scratch_shapes=scratch,
        cost_estimate=pl.CostEstimate(flops=2 * h.shape[0] * width * rows, bytes_accessed=h.shape[0] * width * 2, transcendentals=0),
        compiler_params=pltpu.CompilerParams(vmem_limit_bytes=8 * 2**20),
    )


def products(h, v):
    depth, rows = h.shape
    block = pltpu.VMEM((depth, v.shape[1] // 4), v.dtype)
    slab = pltpu.VMEM((depth, rows), h.dtype)
    total = pltpu.VMEM((v.shape[1] // 4, rows), F32)
    v = streamed(v)
    sems = pltpu.SemaphoreType.DMA((2 * len(cuts(depth)),))

    def opening(ahead):
        kernel = functools.partial(opening_kernel, ahead)
        return kernel_call(kernel, h, v, [HBM, HBM], [slab], [block, total, sems])(streamed(h), v)

    def second(ahead, following, h_here):
        kernel = functools.partial(second_kernel, ahead, following)
        call = kernel_call(kernel, h, v, [VMEM, HBM], [block], [block, total, sems])
        return call(resident(h_here), v)

    def third(following, h_here, v_here):
        kernel = functools.partial(third_kernel, following)
        call = kernel_call(kernel, h, v, [VMEM, VMEM, HBM], [block], [total, sems])
        return call(resident(h_here), resident(v_here), v)

    def closing(h_here, v_here):
        call = kernel_call(closing_kernel, h, v, [VMEM, VMEM], [], [total])
        return call(resident(h_here), resident(v_here))

    return opening, second, third, closing


def near_kernel(*refs):
    own, other, out, sem = refs[:3], refs[3:6], refs[6], refs[7]
    steps = (0, 3, 1)
    write([(ref, step, 0) for ref, step in zip(own, steps)], [(ref, step, 0) for ref, step in zip(other, steps)], out, sem)


def far_kernel(*refs):
    own, other, out, sem = refs[:2], refs[2:4], refs[5], refs[6]
    write([(own[0], 2, 0), (own[1], 2, 1)], [(other[0], 2, 0), (other[1], 2, 1)], out, sem)


def write(own, other, out, sem):
    y, z, core = lax.axis_index("y"), lax.axis_index("z"), lax.axis_index("core")

    def run(first, second):
        made = []
        for ref, step, part in first:
            rows = ref.shape[0]
            column = pl.multiple_of(lax.rem(z + step, 4) * 256, 256)
            made.append((ref, out.at[pl.ds(part * rows, rows), pl.ds(column, 128)]))
        for ref, step, part in second:
            row = pl.multiple_of(lax.rem(y + step, 4) * 256, 256)
            for k in range(ref.shape[0] // 256):
                column = (part * 2 + k) * 256 + 128
                made.append((ref.at[pl.ds(k * 256, 256)], out.at[pl.ds(row, 256), pl.ds(column, 128)]))
        made = [pltpu.make_async_copy(src, dst, sem.at[i]) for i, (src, dst) in enumerate(made)]
        for copy in made:
            copy.start()
        for copy in made:
            copy.wait()

    @pl.when(core == 0)
    def _():
        run(own, other)

    @pl.when(core == 1)
    def _():
        run(other, own)


def place_near(own, other, nvec):
    return pl.pallas_call(
        near_kernel,
        in_specs=[ANY] * 6,
        out_specs=ANY,
        out_shape=jax.ShapeDtypeStruct((nvec, nvec), F32),
        scratch_shapes=[pltpu.SemaphoreType.DMA((15,))],
        compiler_params=pltpu.CompilerParams(vmem_limit_bytes=2**20),
        name="place_near",
    )(*own, *other)


def place_far(own, other, whole):
    return pl.pallas_call(
        far_kernel,
        in_specs=[ANY] * 5,
        out_specs=ANY,
        out_shape=jax.ShapeDtypeStruct(whole.shape, F32),
        input_output_aliases={4: 0},
        scratch_shapes=[pltpu.SemaphoreType.DMA((6,))],
        compiler_params=pltpu.CompilerParams(vmem_limit_bytes=2**20),
        name="place_far",
    )(*own, *other, whole)


def body(h_slab, vectors, left_rows):
    nvec = vectors.shape[1]
    wide = nvec // 8
    half = wide // 2
    opening, second, third, closing = products(h_slab.T, vectors)

    far, give, h_here = opening(2)
    other_far = shift(give, "core", 1)
    up, give, v_next = second(1, 3, h_here)
    other_up = shift(give, "core", 1)
    far = far + other_far
    from_below = shift(far[:half], "z", 1)
    from_above = shift(far[half:], "z", -1)
    down, give, v_next = third(0, h_here, v_next)
    other_down = shift(give, "core", 1)
    up, down = up + other_up, down + other_down
    up = jnp.concatenate([up[:half] + from_below, up[half:]])
    down = jnp.concatenate([down[:half], down[half:] + from_above])
    from_below = shift(up, "z", 1)
    from_above = shift(down, "z", -1)
    own, give = closing(h_here, v_next)
    shared = own + shift(give, "core", 1) + from_below + from_above

    local_part = lax.dot_general(
        left_rows.astype(F32),
        shared,
        (((0,), (1,)), ((), ())),
        precision=lax.Precision.HIGHEST,
        preferred_element_type=F32,
    )
    parts = local_part.reshape(16, nvec // 16, wide)
    parts = lax.all_to_all(parts, PLANE, 0, 0, tiled=True)
    summed = jnp.sum(parts, axis=0)
    copies = jnp.broadcast_to(summed, (16, *summed.shape))
    block = lax.all_to_all(
        copies, AXES, 0, 0, tiled=True, axis_index_groups=plane_groups()
    ).reshape(nvec, wide)

    half = nvec // 2
    below = ring_shift(block, 1)
    above = ring_shift(block, -1)
    other = shift(block, "core", 1)
    far_low = ring_shift(below[:half], 1)
    far_high = ring_shift(above[half:], -1)
    other_below = shift(below, "core", 1)
    other_above = shift(above, "core", 1)
    whole = place_near([block, below, above], [other, other_below, other_above], nvec)
    far = [far_low, far_high]
    return place_far(far, [shift(value, "core", 1) for value in far], whole)


def solution(mesh):
    fine = Mesh(mesh.devices.reshape(SIZES), AXES)
    row, col = ("y", "xh"), ("z", "xl", "core")
    in_specs = (P(row, col), P(col, None), P(row, None))
    return jax.shard_map(body, mesh=fine, in_specs=in_specs, out_specs=P(), check_vma=False)
```

```python
import functools

import jax
import jax.numpy as jnp
from jax import lax
from jax.experimental import pallas as pl
from jax.experimental.pallas import tpu as pltpu
from jax.sharding import Mesh, PartitionSpec as P


AXES = ("y", "xh", "z", "xl", "core")
SIZES = (4, 2, 4, 2, 2)
PLANE = ("y", "xh", "xl")
F32 = jnp.float32
ANY = pl.BlockSpec(memory_space=pl.ANY)
HBM = pl.BlockSpec(memory_space=pltpu.HBM)
VMEM = pl.BlockSpec(memory_space=pltpu.VMEM)


def rank(y, x, z, core):
    return (((y * 2 + x // 2) * 4 + z) * 2 + x % 2) * 2 + core


def shift(value, axis, step):
    size = lax.axis_size(axis)
    return lax.ppermute(value, axis, [(i, (i + step) % size) for i in range(size)])


def ring_shift(value, step):
    pairs = []
    for y in range(4):
        for x in range(4):
            for z in range(4):
                pairs.append((rank(y, x, z, 0), rank(y, x, (z + step) % 4, 0)))
                pairs.append((rank(y, x, z, 1), rank((y + step) % 4, x, z, 1)))
    return lax.ppermute(value, AXES, pairs)


def plane_groups():
    groups = [[rank(y, x, z, 0) for y in range(4) for x in range(4)] for z in range(4)]
    return groups + [[rank(y, x, z, 1) for z in range(4) for x in range(4)] for y in range(4)]


def resident(value):
    return pltpu.with_memory_space_constraint(value, pltpu.VMEM)


def streamed(value):
    return pltpu.with_memory_space_constraint(value, pltpu.HBM)


def cuts(depth):
    return [(start, min(1536, depth - start)) for start in range(0, depth, 1536)]


def multiply(left, right):
    return lax.dot_general(left, right, (((0,), (0,)), ((), ())), preferred_element_type=F32)


def emit(total, keep, give):
    core = lax.axis_index("core")
    rows = total.shape[0] // 2
    keep[...] = total[pl.ds(pl.multiple_of(core * rows, rows), rows), :]
    give[...] = total[pl.ds(pl.multiple_of((1 - core) * rows, rows), rows), :]


def fetch(v, ahead, here, sem, base):
    wide = here.shape[1] // 2
    first = pl.multiple_of(lax.rem(lax.axis_index("z") + ahead, 4) * wide, wide)
    copies = []
    for i, (start, size) in enumerate(cuts(v.shape[0])):
        rows = pl.ds(start, size)
        for k in range(2):
            source = v.at[rows, pl.ds(pl.multiple_of(first + 4 * wide * k, wide), wide)]
            place = here.at[rows, pl.ds(k * wide, wide)]
            copies.append(pltpu.make_async_copy(source, place, sem.at[base + 2 * i + k]))
    return copies


def accumulate(total, v_here, h_here, start, size):
    part = multiply(v_here[start : start + size], h_here[start : start + size])
    if start == 0:
        total[...] = part
    else:
        total[...] += part


def opening_kernel(ahead, h, v, keep, give, h_here, v_here, total, sem):
    spans = cuts(h.shape[0])
    ours = fetch(v, ahead, v_here, sem, 0)
    slab = []
    for i, (start, size) in enumerate(spans):
        rows = pl.ds(start, size)
        slab.append(pltpu.make_async_copy(h.at[rows], h_here.at[rows], sem.at[2 * len(spans) + i]))
    for i in range(len(spans)):
        for copy in (slab[i], ours[2 * i], ours[2 * i + 1]):
            copy.start()
    for i, (start, size) in enumerate(spans):
        for copy in (slab[i], ours[2 * i], ours[2 * i + 1]):
            copy.wait()
        accumulate(total, v_here, h_here, start, size)
    emit(total, keep, give)


def second_kernel(ahead, following, h_here, v, keep, give, v_next, v_here, total, sem):
    spans = cuts(v.shape[0])
    ours = fetch(v, ahead, v_here, sem, 0)
    theirs = fetch(v, following, v_next, sem, 2 * len(spans))
    for copy in (*ours, *theirs):
        copy.start()
    for i, (start, size) in enumerate(spans):
        for copy in (ours[2 * i], ours[2 * i + 1]):
            copy.wait()
        accumulate(total, v_here, h_here, start, size)
    emit(total, keep, give)
    for copy in theirs:
        copy.wait()


def third_kernel(following, h_here, v_here, v, keep, give, v_next, total, sem):
    theirs = fetch(v, following, v_next, sem, 0)
    for copy in theirs:
        copy.start()
    total[...] = multiply(v_here[...], h_here[...])
    emit(total, keep, give)
    for copy in theirs:
        copy.wait()


def closing_kernel(h_here, v_here, keep, give, total):
    total[...] = multiply(v_here[...], h_here[...])
    emit(total, keep, give)


def kernel_call(kernel, h, v, ins, outs, scratch):
    width, rows = v.shape[1] // 4, h.shape[1]
    piece = pltpu.VMEM((width // 2, rows), F32)
    return pl.pallas_call(
        kernel,
        in_specs=ins,
        out_specs=[VMEM] * (2 + len(outs)),
        out_shape=[piece, piece, *outs],
        scratch_shapes=scratch,
        cost_estimate=pl.CostEstimate(flops=2 * h.shape[0] * width * rows, bytes_accessed=h.shape[0] * width * 2, transcendentals=0),
        compiler_params=pltpu.CompilerParams(vmem_limit_bytes=8 * 2**20),
    )


def products(h, v):
    depth, rows = h.shape
    block = pltpu.VMEM((depth, v.shape[1] // 4), v.dtype)
    slab = pltpu.VMEM((depth, rows), h.dtype)
    total = pltpu.VMEM((v.shape[1] // 4, rows), F32)
    v = streamed(v)
    sems = pltpu.SemaphoreType.DMA((4 * len(cuts(depth)),))

    def opening(ahead):
        kernel = functools.partial(opening_kernel, ahead)
        return kernel_call(kernel, h, v, [HBM, HBM], [slab], [block, total, sems])(streamed(h), v)

    def second(ahead, following, h_here):
        kernel = functools.partial(second_kernel, ahead, following)
        call = kernel_call(kernel, h, v, [VMEM, HBM], [block], [block, total, sems])
        return call(resident(h_here), v)

    def third(following, h_here, v_here):
        kernel = functools.partial(third_kernel, following)
        call = kernel_call(kernel, h, v, [VMEM, VMEM, HBM], [block], [total, sems])
        return call(resident(h_here), resident(v_here), v)

    def closing(h_here, v_here):
        call = kernel_call(closing_kernel, h, v, [VMEM, VMEM], [], [total])
        return call(resident(h_here), resident(v_here))

    return opening, second, third, closing


def near_kernel(*refs):
    own, other, out, sem = refs[:3], refs[3:6], refs[6], refs[7]
    steps = (0, 3, 1)
    write([(ref, step, 0) for ref, step in zip(own, steps)], [(ref, step, 0) for ref, step in zip(other, steps)], out, sem)


def far_kernel(*refs):
    own, other, out, sem = refs[:2], refs[2:4], refs[5], refs[6]
    write([(own[0], 2, 0), (own[1], 2, 1)], [(other[0], 2, 0), (other[1], 2, 1)], out, sem)


def write(own, other, out, sem):
    y, z, core = lax.axis_index("y"), lax.axis_index("z"), lax.axis_index("core")

    def run(first, second):
        made = []
        for ref, step, part in first:
            rows = ref.shape[0]
            column = pl.multiple_of(lax.rem(z + step, 4) * 128, 128)
            made.append((ref, out.at[pl.ds(part * rows, rows), pl.ds(column, 128)]))
        for ref, step, part in second:
            row = pl.multiple_of(lax.rem(y + step, 4) * 256, 256)
            for k in range(ref.shape[0] // 256):
                column = 512 + (part * 2 + k) * 128
                made.append((ref.at[pl.ds(k * 256, 256)], out.at[pl.ds(row, 256), pl.ds(column, 128)]))
        made = [pltpu.make_async_copy(src, dst, sem.at[i]) for i, (src, dst) in enumerate(made)]
        for copy in made:
            copy.start()
        for copy in made:
            copy.wait()

    @pl.when(core == 0)
    def _():
        run(own, other)

    @pl.when(core == 1)
    def _():
        run(other, own)


def place_near(own, other, nvec):
    return pl.pallas_call(
        near_kernel,
        in_specs=[ANY] * 6,
        out_specs=ANY,
        out_shape=jax.ShapeDtypeStruct((nvec, nvec), F32),
        scratch_shapes=[pltpu.SemaphoreType.DMA((15,))],
        compiler_params=pltpu.CompilerParams(vmem_limit_bytes=2**20),
        name="place_near",
    )(*own, *other)


def place_far(own, other, whole):
    return pl.pallas_call(
        far_kernel,
        in_specs=[ANY] * 5,
        out_specs=ANY,
        out_shape=jax.ShapeDtypeStruct(whole.shape, F32),
        input_output_aliases={4: 0},
        scratch_shapes=[pltpu.SemaphoreType.DMA((6,))],
        compiler_params=pltpu.CompilerParams(vmem_limit_bytes=2**20),
        name="place_far",
    )(*own, *other, whole)


def body(h_slab, vectors, left_rows):
    nvec = vectors.shape[1]
    wide = nvec // 8
    half = wide // 2
    opening, second, third, closing = products(h_slab.T, vectors)

    far, give, h_here = opening(2)
    other_far = shift(give, "core", 1)
    up, give, v_next = second(1, 3, h_here)
    other_up = shift(give, "core", 1)
    far = far + other_far
    from_below = shift(far[:half], "z", 1)
    from_above = shift(far[half:], "z", -1)
    down, give, v_next = third(0, h_here, v_next)
    other_down = shift(give, "core", 1)
    up, down = up + other_up, down + other_down
    up = jnp.concatenate([up[:half] + from_below, up[half:]])
    down = jnp.concatenate([down[:half], down[half:] + from_above])
    from_below = shift(up, "z", 1)
    from_above = shift(down, "z", -1)
    own, give = closing(h_here, v_next)
    shared = own + shift(give, "core", 1) + from_below + from_above

    local_part = lax.dot_general(
        left_rows.astype(F32),
        shared,
        (((0,), (1,)), ((), ())),
        precision=lax.Precision.HIGHEST,
        preferred_element_type=F32,
    )
    parts = local_part.reshape(16, nvec // 16, wide)
    parts = lax.all_to_all(parts, PLANE, 0, 0, tiled=True)
    summed = jnp.sum(parts, axis=0)
    copies = jnp.broadcast_to(summed, (16, *summed.shape))
    block = lax.all_to_all(
        copies, AXES, 0, 0, tiled=True, axis_index_groups=plane_groups()
    ).reshape(nvec, wide)

    half = nvec // 2
    below = ring_shift(block, 1)
    above = ring_shift(block, -1)
    other = shift(block, "core", 1)
    far_low = ring_shift(below[:half], 1)
    far_high = ring_shift(above[half:], -1)
    other_below = shift(below, "core", 1)
    other_above = shift(above, "core", 1)
    whole = place_near([block, below, above], [other, other_below, other_above], nvec)
    far = [far_low, far_high]
    return place_far(far, [shift(value, "core", 1) for value in far], whole)


def solution(mesh):
    fine = Mesh(mesh.devices.reshape(SIZES), AXES)
    row, col = ("y", "xh"), ("z", "xl", "core")
    in_specs = (P(row, col), P(col, None), P(row, None))
    return jax.shard_map(body, mesh=fine, in_specs=in_specs, out_specs=P(), check_vma=False)
```

```python
import functools

import jax
import jax.numpy as jnp
from jax import lax
from jax.experimental import pallas as pl
from jax.experimental.pallas import tpu as pltpu
from jax.sharding import Mesh, PartitionSpec as P


AXES = ("y", "xh", "z", "xl", "core")
SIZES = (4, 2, 4, 2, 2)
PLANE = ("y", "xh", "xl")
F32 = jnp.float32
ANY = pl.BlockSpec(memory_space=pl.ANY)
HBM = pl.BlockSpec(memory_space=pltpu.HBM)
VMEM = pl.BlockSpec(memory_space=pltpu.VMEM)


def rank(y, x, z, core):
    return (((y * 2 + x // 2) * 4 + z) * 2 + x % 2) * 2 + core


def shift(value, axis, step):
    size = lax.axis_size(axis)
    return lax.ppermute(value, axis, [(i, (i + step) % size) for i in range(size)])


def ring_shift(value, step):
    pairs = []
    for y in range(4):
        for x in range(4):
            for z in range(4):
                pairs.append((rank(y, x, z, 0), rank(y, x, (z + step) % 4, 0)))
                pairs.append((rank(y, x, z, 1), rank((y + step) % 4, x, z, 1)))
    return lax.ppermute(value, AXES, pairs)


def plane_groups():
    groups = [[rank(y, x, z, 0) for y in range(4) for x in range(4)] for z in range(4)]
    return groups + [[rank(y, x, z, 1) for z in range(4) for x in range(4)] for y in range(4)]


def resident(value):
    return pltpu.with_memory_space_constraint(value, pltpu.VMEM)


def streamed(value):
    return pltpu.with_memory_space_constraint(value, pltpu.HBM)


def cuts(depth):
    return [(start, min(1536, depth - start)) for start in range(0, depth, 1536)]


def multiply(left, right):
    return lax.dot_general(left, right, (((0,), (0,)), ((), ())), preferred_element_type=F32)


def columns_of(v, ahead, rows):
    width = v.shape[1] // 4
    column = pl.multiple_of(lax.rem(lax.axis_index("z") + ahead, 4) * width, width)
    return v.at[rows, pl.ds(column, width)]


def emit(total, keep, give):
    core = lax.axis_index("core")
    rows = total.shape[0] // 2
    keep[...] = total[pl.ds(pl.multiple_of(core * rows, rows), rows), :]
    give[...] = total[pl.ds(pl.multiple_of((1 - core) * rows, rows), rows), :]


def fetch(v, ahead, here, sem, base):
    copies = []
    for i, (start, size) in enumerate(cuts(v.shape[0])):
        rows = pl.ds(start, size)
        copies.append(pltpu.make_async_copy(columns_of(v, ahead, rows), here.at[rows], sem.at[base + i]))
    return copies


def accumulate(total, v_here, h_here, start, size):
    part = multiply(v_here[start : start + size], h_here[start : start + size])
    if start == 0:
        total[...] = part
    else:
        total[...] += part


def opening_kernel(ahead, h, v, keep, give, h_here, v_here, total, sem):
    spans = cuts(h.shape[0])
    ours = fetch(v, ahead, v_here, sem, 0)
    slab = []
    for i, (start, size) in enumerate(spans):
        rows = pl.ds(start, size)
        slab.append(pltpu.make_async_copy(h.at[rows], h_here.at[rows], sem.at[len(spans) + i]))
    for one, two in zip(slab, ours):
        one.start()
        two.start()
    for (start, size), one, two in zip(spans, slab, ours):
        one.wait()
        two.wait()
        accumulate(total, v_here, h_here, start, size)
    emit(total, keep, give)


def second_kernel(ahead, following, h_here, v, keep, give, v_next, v_here, total, sem):
    spans = cuts(v.shape[0])
    ours = fetch(v, ahead, v_here, sem, 0)
    theirs = fetch(v, following, v_next, sem, len(spans))
    for copy in (*ours, *theirs):
        copy.start()
    for (start, size), copy in zip(spans, ours):
        copy.wait()
        accumulate(total, v_here, h_here, start, size)
    emit(total, keep, give)
    for copy in theirs:
        copy.wait()


def third_kernel(following, h_here, v_here, v, keep, give, v_next, total, sem):
    theirs = fetch(v, following, v_next, sem, 0)
    for copy in theirs:
        copy.start()
    step = v.shape[0] // 3
    total[...] = jnp.zeros_like(total)

    @pl.loop(0, 3)
    def _(i):
        rows = pl.ds(pl.multiple_of(i * step, 16), step)
        total[...] += multiply(v_here[rows, :], h_here[rows, :])

    emit(total, keep, give)
    for copy in theirs:
        copy.wait()


def closing_kernel(h_here, v_here, keep, give, total):
    total[...] = multiply(v_here[...], h_here[...])
    emit(total, keep, give)


def kernel_call(kernel, h, v, ins, outs, scratch):
    width, rows = v.shape[1] // 4, h.shape[1]
    piece = pltpu.VMEM((width // 2, rows), F32)
    return pl.pallas_call(
        kernel,
        in_specs=ins,
        out_specs=[VMEM] * (2 + len(outs)),
        out_shape=[piece, piece, *outs],
        scratch_shapes=scratch,
        cost_estimate=pl.CostEstimate(flops=2 * h.shape[0] * width * rows, bytes_accessed=h.shape[0] * width * 2, transcendentals=0),
        compiler_params=pltpu.CompilerParams(vmem_limit_bytes=8 * 2**20),
    )


def products(h, v):
    depth, rows = h.shape
    block = pltpu.VMEM((depth, v.shape[1] // 4), v.dtype)
    slab = pltpu.VMEM((depth, rows), h.dtype)
    total = pltpu.VMEM((v.shape[1] // 4, rows), F32)
    v = streamed(v)
    sems = pltpu.SemaphoreType.DMA((2 * len(cuts(depth)),))

    def opening(ahead):
        kernel = functools.partial(opening_kernel, ahead)
        return kernel_call(kernel, h, v, [HBM, HBM], [slab], [block, total, sems])(streamed(h), v)

    def second(ahead, following, h_here):
        kernel = functools.partial(second_kernel, ahead, following)
        call = kernel_call(kernel, h, v, [VMEM, HBM], [block], [block, total, sems])
        return call(resident(h_here), v)

    def third(following, h_here, v_here):
        kernel = functools.partial(third_kernel, following)
        call = kernel_call(kernel, h, v, [VMEM, VMEM, HBM], [block], [total, sems])
        return call(resident(h_here), resident(v_here), v)

    def closing(h_here, v_here):
        call = kernel_call(closing_kernel, h, v, [VMEM, VMEM], [], [total])
        return call(resident(h_here), resident(v_here))

    return opening, second, third, closing


def near_kernel(*refs):
    own, other, out, sem = refs[:5], refs[5:10], refs[10], refs[11]
    spots = ((0, None), (3, 0), (3, 1), (1, 0), (1, 1))

    def spread(blocks):
        return [(ref, step, part) for ref, (step, part) in zip(blocks, spots)]

    write(spread(own), spread(other), out, sem)


def far_kernel(*refs):
    own, other, out, sem = refs[:2], refs[2:4], refs[5], refs[6]
    write([(own[0], 2, 0), (own[1], 2, 1)], [(other[0], 2, 0), (other[1], 2, 1)], out, sem)


def write(own, other, out, sem):
    y, z, core = lax.axis_index("y"), lax.axis_index("z"), lax.axis_index("core")

    def run(first, second):
        made = []
        for ref, step, part in first:
            rows, part = ref.shape[0], part or 0
            column = pl.multiple_of(lax.rem(z + step, 4) * 256, 256)
            made.append((ref, out.at[pl.ds(part * rows, rows), pl.ds(column, 128)]))
        for ref, step, part in second:
            part = part or 0
            row = pl.multiple_of(lax.rem(y + step, 4) * 256, 256)
            for k in range(ref.shape[0] // 256):
                column = (part * 2 + k) * 256 + 128
                made.append((ref.at[pl.ds(k * 256, 256)], out.at[pl.ds(row, 256), pl.ds(column, 128)]))
        made = [pltpu.make_async_copy(src, dst, sem.at[i]) for i, (src, dst) in enumerate(made)]
        for copy in made:
            copy.start()
        for copy in made:
            copy.wait()

    @pl.when(core == 0)
    def _():
        run(own, other)

    @pl.when(core == 1)
    def _():
        run(other, own)


def place_near(own, other, nvec):
    return pl.pallas_call(
        near_kernel,
        in_specs=[ANY] * 10,
        out_specs=ANY,
        out_shape=jax.ShapeDtypeStruct((nvec, nvec), F32),
        scratch_shapes=[pltpu.SemaphoreType.DMA((17,))],
        compiler_params=pltpu.CompilerParams(vmem_limit_bytes=2**20),
        name="place_near",
    )(*own, *other)


def place_far(own, other, whole):
    return pl.pallas_call(
        far_kernel,
        in_specs=[ANY] * 5,
        out_specs=ANY,
        out_shape=jax.ShapeDtypeStruct(whole.shape, F32),
        input_output_aliases={4: 0},
        scratch_shapes=[pltpu.SemaphoreType.DMA((6,))],
        compiler_params=pltpu.CompilerParams(vmem_limit_bytes=2**20),
        name="place_far",
    )(*own, *other, whole)


def body(h_slab, vectors, left_rows):
    nvec = vectors.shape[1]
    wide = nvec // 8
    half = wide // 2
    opening, second, third, closing = products(h_slab.T, vectors)

    far, give, h_here = opening(2)
    other_far = shift(give, "core", 1)
    up, give, v_next = second(1, 3, h_here)
    other_up = shift(give, "core", 1)
    far = far + other_far
    from_below = shift(far[:half], "z", 1)
    from_above = shift(far[half:], "z", -1)
    down, give, v_next = third(0, h_here, v_next)
    other_down = shift(give, "core", 1)
    up, down = up + other_up, down + other_down
    up = jnp.concatenate([up[:half] + from_below, up[half:]])
    down = jnp.concatenate([down[:half], down[half:] + from_above])
    from_below = shift(up, "z", 1)
    from_above = shift(down, "z", -1)
    own, give = closing(h_here, v_next)
    shared = own + shift(give, "core", 1) + from_below + from_above

    local_part = lax.dot_general(
        left_rows.astype(F32),
        shared,
        (((0,), (1,)), ((), ())),
        precision=lax.Precision.HIGHEST,
        preferred_element_type=F32,
    )
    parts = local_part.reshape(16, nvec // 16, wide)
    parts = lax.all_to_all(parts, PLANE, 0, 0, tiled=True)
    summed = jnp.sum(parts, axis=0)
    copies = jnp.broadcast_to(summed, (16, *summed.shape))
    block = lax.all_to_all(
        copies, AXES, 0, 0, tiled=True, axis_index_groups=plane_groups()
    ).reshape(nvec, wide)

    low, high = block[: nvec // 2], block[nvec // 2 :]
    below_low = ring_shift(low, 1)
    above_high = ring_shift(high, -1)
    below_high = ring_shift(high, 1)
    above_low = ring_shift(low, -1)
    far_low = ring_shift(below_low, 1)
    far_high = ring_shift(above_high, -1)
    other = shift(block, "core", 1)
    near = [below_low, below_high, above_low, above_high]
    other_near = [shift(value, "core", 1) for value in near]
    whole = place_near([block, *near], [other, *other_near], nvec)
    far = [far_low, far_high]
    return place_far(far, [shift(value, "core", 1) for value in far], whole)


def solution(mesh):
    fine = Mesh(mesh.devices.reshape(SIZES), AXES)
    row, col = ("y", "xh"), ("z", "xl", "core")
    in_specs = (P(row, col), P(col, None), P(row, None))
    return jax.shard_map(body, mesh=fine, in_specs=in_specs, out_specs=P(), check_vma=False)
```

```python
import functools

import jax
import jax.numpy as jnp
from jax import lax
from jax.experimental import pallas as pl
from jax.experimental.pallas import tpu as pltpu
from jax.sharding import Mesh, PartitionSpec as P


AXES = ("y", "xh", "z", "xl", "core")
SIZES = (4, 2, 4, 2, 2)
PLANE = ("y", "xh", "xl")
F32 = jnp.float32
ANY = pl.BlockSpec(memory_space=pl.ANY)
HBM = pl.BlockSpec(memory_space=pltpu.HBM)
VMEM = pl.BlockSpec(memory_space=pltpu.VMEM)


def rank(y, x, z, core):
    return (((y * 2 + x // 2) * 4 + z) * 2 + x % 2) * 2 + core


def shift(value, axis, step):
    size = lax.axis_size(axis)
    return lax.ppermute(value, axis, [(i, (i + step) % size) for i in range(size)])


def cross_z(value, step):
    pairs = []
    for y in range(4):
        for x in range(4):
            for z in range(4):
                for core in range(2):
                    pairs.append((rank(y, x, z, core), rank(y, x, (z + step) % 4, 1 - core)))
    return lax.ppermute(value, AXES, pairs)


def ring_shift(value, step, holder):
    pairs = []
    for y in range(4):
        for x in range(4):
            for z in range(4):
                pairs.append((rank(y, x, z, holder), rank(y, x, (z + step) % 4, 1 - holder)))
                pairs.append((rank(y, x, z, 1 - holder), rank((y + step) % 4, x, z, holder)))
    return lax.ppermute(value, AXES, pairs)


def plane_groups():
    groups = [[rank(y, x, z, 0) for y in range(4) for x in range(4)] for z in range(4)]
    return groups + [[rank(y, x, z, 1) for z in range(4) for x in range(4)] for y in range(4)]


def resident(value):
    return pltpu.with_memory_space_constraint(value, pltpu.VMEM)


def streamed(value):
    return pltpu.with_memory_space_constraint(value, pltpu.HBM)


def cuts(depth):
    return [(start, min(1536, depth - start)) for start in range(0, depth, 1536)]


def multiply(left, right):
    return lax.dot_general(left, right, (((0,), (0,)), ((), ())), preferred_element_type=F32)


def columns_of(v, ahead, rows):
    width = v.shape[1] // 4
    column = pl.multiple_of(lax.rem(lax.axis_index("z") + ahead, 4) * width, width)
    return v.at[rows, pl.ds(column, width)]


def emit(total, keep, give):
    side = lax.rem(lax.axis_index("core") + lax.axis_index("z"), 2)
    rows = total.shape[0] // 2
    keep[...] = total[pl.ds(pl.multiple_of(side * rows, rows), rows), :]
    give[...] = total[pl.ds(pl.multiple_of((1 - side) * rows, rows), rows), :]


def fetch(v, ahead, here, sem, base):
    copies = []
    for i, (start, size) in enumerate(cuts(v.shape[0])):
        rows = pl.ds(start, size)
        copies.append(pltpu.make_async_copy(columns_of(v, ahead, rows), here.at[rows], sem.at[base + i]))
    return copies


def accumulate(total, v_here, h_here, start, size):
    part = multiply(v_here[start : start + size], h_here[start : start + size])
    if start == 0:
        total[...] = part
    else:
        total[...] += part


def opening_kernel(ahead, h, v, keep, give, h_here, v_here, total, sem):
    spans = cuts(h.shape[0])
    ours = fetch(v, ahead, v_here, sem, 0)
    slab = []
    for i, (start, size) in enumerate(spans):
        rows = pl.ds(start, size)
        slab.append(pltpu.make_async_copy(h.at[rows], h_here.at[rows], sem.at[len(spans) + i]))
    for one, two in zip(slab, ours):
        one.start()
        two.start()
    for (start, size), one, two in zip(spans, slab, ours):
        one.wait()
        two.wait()
        accumulate(total, v_here, h_here, start, size)
    emit(total, keep, give)


def second_kernel(ahead, following, h_here, v, keep, give, v_next, v_here, total, sem):
    spans = cuts(v.shape[0])
    ours = fetch(v, ahead, v_here, sem, 0)
    theirs = fetch(v, following, v_next, sem, len(spans))
    for copy in (*ours, *theirs):
        copy.start()
    for (start, size), copy in zip(spans, ours):
        copy.wait()
        accumulate(total, v_here, h_here, start, size)
    emit(total, keep, give)
    for copy in theirs:
        copy.wait()


def third_kernel(following, h_here, v_here, v, keep, give, v_next, total, sem):
    theirs = fetch(v, following, v_next, sem, 0)
    for copy in theirs:
        copy.start()
    step = v.shape[0] // 3
    total[...] = jnp.zeros_like(total)

    @pl.loop(0, 3)
    def _(i):
        rows = pl.ds(pl.multiple_of(i * step, 16), step)
        total[...] += multiply(v_here[rows, :], h_here[rows, :])

    emit(total, keep, give)
    for copy in theirs:
        copy.wait()


def closing_kernel(h_here, v_here, keep, give, total):
    total[...] = multiply(v_here[...], h_here[...])
    emit(total, keep, give)


def kernel_call(kernel, h, v, ins, outs, scratch):
    width, rows = v.shape[1] // 4, h.shape[1]
    piece = pltpu.VMEM((width // 2, rows), F32)
    return pl.pallas_call(
        kernel,
        in_specs=ins,
        out_specs=[VMEM] * (2 + len(outs)),
        out_shape=[piece, piece, *outs],
        scratch_shapes=scratch,
        cost_estimate=pl.CostEstimate(flops=2 * h.shape[0] * width * rows, bytes_accessed=h.shape[0] * width * 2, transcendentals=0),
        compiler_params=pltpu.CompilerParams(vmem_limit_bytes=8 * 2**20),
    )


def products(h, v):
    depth, rows = h.shape
    block = pltpu.VMEM((depth, v.shape[1] // 4), v.dtype)
    slab = pltpu.VMEM((depth, rows), h.dtype)
    total = pltpu.VMEM((v.shape[1] // 4, rows), F32)
    v = streamed(v)
    sems = pltpu.SemaphoreType.DMA((2 * len(cuts(depth)),))

    def opening(ahead):
        kernel = functools.partial(opening_kernel, ahead)
        return kernel_call(kernel, h, v, [HBM, HBM], [slab], [block, total, sems])(streamed(h), v)

    def second(ahead, following, h_here):
        kernel = functools.partial(second_kernel, ahead, following)
        call = kernel_call(kernel, h, v, [VMEM, HBM], [block], [block, total, sems])
        return call(resident(h_here), v)

    def third(following, h_here, v_here):
        kernel = functools.partial(third_kernel, following)
        call = kernel_call(kernel, h, v, [VMEM, VMEM, HBM], [block], [total, sems])
        return call(resident(h_here), resident(v_here), v)

    def closing(h_here, v_here):
        call = kernel_call(closing_kernel, h, v, [VMEM, VMEM], [], [total])
        return call(resident(h_here), resident(v_here))

    return opening, second, third, closing


def near_kernel(*refs):
    own, other, out, sem = refs[:5], refs[5:10], refs[10], refs[11]
    spots = ((0, None), (3, 0), (3, 1), (1, 0), (1, 1))

    def spread(blocks):
        return [(ref, step, part) for ref, (step, part) in zip(blocks, spots)]

    write(spread(own), spread(other), out, sem)


def far_kernel(*refs):
    own, other, out, sem = refs[:2], refs[2:4], refs[5], refs[6]
    write([(own[0], 2, 0), (own[1], 2, 1)], [(other[0], 2, 0), (other[1], 2, 1)], out, sem)


def write(own, other, out, sem):
    y, z, core = lax.axis_index("y"), lax.axis_index("z"), lax.axis_index("core")

    def run(first, second):
        made = []
        for ref, step, part in first:
            rows, part = ref.shape[0], part or 0
            there = lax.rem(z + step, 4)
            column = pl.multiple_of(there * 256 + lax.rem(there, 2) * 128, 128)
            made.append((ref, out.at[pl.ds(part * rows, rows), pl.ds(column, 128)]))
        for ref, step, part in second:
            part = part or 0
            row = pl.multiple_of(lax.rem(y + step, 4) * 256, 256)
            for k in range(ref.shape[0] // 256):
                there = part * 2 + k
                column = there * 256 + (1 - there % 2) * 128
                made.append((ref.at[pl.ds(k * 256, 256)], out.at[pl.ds(row, 256), pl.ds(column, 128)]))
        made = [pltpu.make_async_copy(src, dst, sem.at[i]) for i, (src, dst) in enumerate(made)]
        for copy in made:
            copy.start()
        for copy in made:
            copy.wait()

    @pl.when(core == 0)
    def _():
        run(own, other)

    @pl.when(core == 1)
    def _():
        run(other, own)


def place_near(own, other, nvec):
    return pl.pallas_call(
        near_kernel,
        in_specs=[ANY] * 10,
        out_specs=ANY,
        out_shape=jax.ShapeDtypeStruct((nvec, nvec), F32),
        scratch_shapes=[pltpu.SemaphoreType.DMA((17,))],
        compiler_params=pltpu.CompilerParams(vmem_limit_bytes=2**20),
        name="place_near",
    )(*own, *other)


def place_far(own, other, whole):
    return pl.pallas_call(
        far_kernel,
        in_specs=[ANY] * 5,
        out_specs=ANY,
        out_shape=jax.ShapeDtypeStruct(whole.shape, F32),
        input_output_aliases={4: 0},
        scratch_shapes=[pltpu.SemaphoreType.DMA((6,))],
        compiler_params=pltpu.CompilerParams(vmem_limit_bytes=2**20),
        name="place_far",
    )(*own, *other, whole)


def body(h_slab, vectors, left_rows):
    nvec = vectors.shape[1]
    wide = nvec // 8
    half = wide // 2
    opening, second, third, closing = products(h_slab.T, vectors)

    far, give, h_here = opening(2)
    other_far = shift(give, "core", 1)
    up, give, v_next = second(1, 3, h_here)
    other_up = shift(give, "core", 1)
    far = far + other_far
    from_below = cross_z(far[:half], 1)
    from_above = cross_z(far[half:], -1)
    down, give, v_next = third(0, h_here, v_next)
    other_down = shift(give, "core", 1)
    up, down = up + other_up, down + other_down
    up = jnp.concatenate([up[:half] + from_below, up[half:]])
    down = jnp.concatenate([down[:half], down[half:] + from_above])
    from_below = cross_z(up, 1)
    from_above = cross_z(down, -1)
    own, give = closing(h_here, v_next)
    shared = own + shift(give, "core", 1) + from_below + from_above

    local_part = lax.dot_general(
        left_rows.astype(F32),
        shared,
        (((0,), (1,)), ((), ())),
        precision=lax.Precision.HIGHEST,
        preferred_element_type=F32,
    )
    parts = local_part.reshape(16, nvec // 16, wide)
    parts = lax.all_to_all(parts, PLANE, 0, 0, tiled=True)
    summed = jnp.sum(parts, axis=0)
    copies = jnp.broadcast_to(summed, (16, *summed.shape))
    block = lax.all_to_all(
        copies, AXES, 0, 0, tiled=True, axis_index_groups=plane_groups()
    ).reshape(nvec, wide)

    low, high = block[: nvec // 2], block[nvec // 2 :]
    below_low = ring_shift(low, 1, 0)
    above_high = ring_shift(high, -1, 0)
    below_high = ring_shift(high, 1, 0)
    above_low = ring_shift(low, -1, 0)
    far_low = ring_shift(below_low, 1, 1)
    far_high = ring_shift(above_high, -1, 1)
    other = shift(block, "core", 1)
    near = [below_low, below_high, above_low, above_high]
    other_near = [shift(value, "core", 1) for value in near]
    whole = place_near([block, *other_near], [other, *near], nvec)
    far = [far_low, far_high]
    return place_far(far, [shift(value, "core", 1) for value in far], whole)


def solution(mesh):
    fine = Mesh(mesh.devices.reshape(SIZES), AXES)
    row, col = ("y", "xh"), ("z", "xl", "core")
    in_specs = (P(row, col), P(col, None), P(row, None))
    return jax.shard_map(body, mesh=fine, in_specs=in_specs, out_specs=P(), check_vma=False)
```

```python
import functools

import jax
import jax.numpy as jnp
from jax import lax
from jax.experimental import pallas as pl
from jax.experimental.pallas import tpu as pltpu
from jax.sharding import Mesh, PartitionSpec as P


AXES = ("y", "xh", "z", "xl", "core")
SIZES = (4, 2, 4, 2, 2)
PLANE = ("y", "xh", "xl")
F32 = jnp.float32
ANY = pl.BlockSpec(memory_space=pl.ANY)
HBM = pl.BlockSpec(memory_space=pltpu.HBM)
VMEM = pl.BlockSpec(memory_space=pltpu.VMEM)


def rank(y, x, z, core):
    return (((y * 2 + x // 2) * 4 + z) * 2 + x % 2) * 2 + core


def shift(value, axis, step):
    size = lax.axis_size(axis)
    return lax.ppermute(value, axis, [(i, (i + step) % size) for i in range(size)])


def ring_shift(value, step):
    pairs = []
    for y in range(4):
        for x in range(4):
            for z in range(4):
                pairs.append((rank(y, x, z, 0), rank(y, x, (z + step) % 4, 0)))
                pairs.append((rank(y, x, z, 1), rank((y + step) % 4, x, z, 1)))
    return lax.ppermute(value, AXES, pairs)


def plane_groups():
    groups = [[rank(y, x, z, 0) for y in range(4) for x in range(4)] for z in range(4)]
    return groups + [[rank(y, x, z, 1) for z in range(4) for x in range(4)] for y in range(4)]


def resident(value):
    return pltpu.with_memory_space_constraint(value, pltpu.VMEM)


def streamed(value):
    return pltpu.with_memory_space_constraint(value, pltpu.HBM)


def cuts(depth):
    return [(start, min(1536, depth - start)) for start in range(0, depth, 1536)]


def multiply(left, right):
    return lax.dot_general(left, right, (((0,), (0,)), ((), ())), preferred_element_type=F32)


def columns_of(v, ahead, rows):
    width = v.shape[1] // 4
    column = pl.multiple_of(lax.rem(lax.axis_index("z") + ahead, 4) * width, width)
    return v.at[rows, pl.ds(column, width)]


def emit(total, keep, give):
    core = lax.axis_index("core")
    rows = total.shape[0] // 2
    keep[...] = total[pl.ds(pl.multiple_of(core * rows, rows), rows), :]
    give[...] = total[pl.ds(pl.multiple_of((1 - core) * rows, rows), rows), :]


def fetch(v, ahead, here, sem, base):
    copies = []
    for i, (start, size) in enumerate(cuts(v.shape[0])):
        rows = pl.ds(start, size)
        copies.append(pltpu.make_async_copy(columns_of(v, ahead, rows), here.at[rows], sem.at[base + i]))
    return copies


def accumulate(total, v_here, h_here, start, size):
    part = multiply(v_here[start : start + size], h_here[start : start + size])
    if start == 0:
        total[...] = part
    else:
        total[...] += part


def opening_kernel(ahead, h, v, keep, give, h_here, v_here, total, sem):
    spans = cuts(h.shape[0])
    ours = fetch(v, ahead, v_here, sem, 0)
    slab = []
    for i, (start, size) in enumerate(spans):
        rows = pl.ds(start, size)
        slab.append(pltpu.make_async_copy(h.at[rows], h_here.at[rows], sem.at[len(spans) + i]))
    for one, two in zip(slab, ours):
        one.start()
        two.start()
    for (start, size), one, two in zip(spans, slab, ours):
        one.wait()
        two.wait()
        accumulate(total, v_here, h_here, start, size)
    emit(total, keep, give)


def second_kernel(ahead, following, h_here, v, keep, give, v_next, v_here, total, sem):
    spans = cuts(v.shape[0])
    ours = fetch(v, ahead, v_here, sem, 0)
    theirs = fetch(v, following, v_next, sem, len(spans))
    for copy in (*ours, *theirs):
        copy.start()
    for (start, size), copy in zip(spans, ours):
        copy.wait()
        accumulate(total, v_here, h_here, start, size)
    emit(total, keep, give)
    for copy in theirs:
        copy.wait()


def third_kernel(h_here, v_here, keep, give, total):
    total[...] = multiply(v_here[...], h_here[...])
    emit(total, keep, give)


def closing_kernel(ahead, h_here, v, keep, give, v_here, total, sem):
    spans = cuts(v.shape[0])
    ours = fetch(v, ahead, v_here, sem, 0)
    for copy in ours:
        copy.start()
    for (start, size), copy in zip(spans, ours):
        copy.wait()
        accumulate(total, v_here, h_here, start, size)
    emit(total, keep, give)


def kernel_call(kernel, h, v, ins, outs, scratch):
    width, rows = v.shape[1] // 4, h.shape[1]
    piece = pltpu.VMEM((width // 2, rows), F32)
    return pl.pallas_call(
        kernel,
        in_specs=ins,
        out_specs=[VMEM] * (2 + len(outs)),
        out_shape=[piece, piece, *outs],
        scratch_shapes=scratch,
        cost_estimate=pl.CostEstimate(flops=2 * h.shape[0] * width * rows, bytes_accessed=h.shape[0] * width * 2, transcendentals=0),
        compiler_params=pltpu.CompilerParams(vmem_limit_bytes=8 * 2**20),
    )


def products(h, v):
    depth, rows = h.shape
    block = pltpu.VMEM((depth, v.shape[1] // 4), v.dtype)
    slab = pltpu.VMEM((depth, rows), h.dtype)
    total = pltpu.VMEM((v.shape[1] // 4, rows), F32)
    v = streamed(v)
    sems = pltpu.SemaphoreType.DMA((2 * len(cuts(depth)),))

    def opening(ahead):
        kernel = functools.partial(opening_kernel, ahead)
        return kernel_call(kernel, h, v, [HBM, HBM], [slab], [block, total, sems])(streamed(h), v)

    def second(ahead, following, h_here):
        kernel = functools.partial(second_kernel, ahead, following)
        call = kernel_call(kernel, h, v, [VMEM, HBM], [block], [block, total, sems])
        return call(resident(h_here), v)

    def third(h_here, v_here):
        call = kernel_call(third_kernel, h, v, [VMEM, VMEM], [], [total])
        return call(resident(h_here), resident(v_here))

    def closing(ahead, h_here):
        kernel = functools.partial(closing_kernel, ahead)
        call = kernel_call(kernel, h, v, [VMEM, HBM], [], [block, total, sems])
        return call(resident(h_here), v)

    return opening, second, third, closing


def place_kernel(own_spots, other_spots, count, *refs):
    own = list(zip(refs[: len(own_spots)], own_spots))
    other = list(zip(refs[len(own_spots) : len(own_spots) + len(other_spots)], other_spots))
    write([(ref, *spot) for ref, spot in own], [(ref, *spot) for ref, spot in other], refs[count], refs[count + 1])


def write(own, other, out, sem):
    y, z, core = lax.axis_index("y"), lax.axis_index("z"), lax.axis_index("core")

    def run(first, second):
        made = []
        for ref, step, part in first:
            rows = ref.shape[0]
            column = pl.multiple_of(lax.rem(z + step, 4) * 256, 256)
            made.append((ref, out.at[pl.ds(part * rows, rows), pl.ds(column, 128)]))
        for ref, step, part in second:
            row = pl.multiple_of(lax.rem(y + step, 4) * 256, 256)
            for k in range(ref.shape[0] // 256):
                column = (part * 2 + k) * 256 + 128
                made.append((ref.at[pl.ds(k * 256, 256)], out.at[pl.ds(row, 256), pl.ds(column, 128)]))
        made = [pltpu.make_async_copy(src, dst, sem.at[i]) for i, (src, dst) in enumerate(made)]
        for copy in made:
            copy.start()
        for copy in made:
            copy.wait()

    @pl.when(core == 0)
    def _():
        run(own, other)

    @pl.when(core == 1)
    def _():
        run(other, own)


def place(own, other, whole, nvec):
    blocks = [block for block, *_ in (*own, *other)]
    earlier = [] if whole is None else [whole]
    count = len(blocks) + len(earlier)
    kernel = functools.partial(
        place_kernel, [tuple(spot) for _, *spot in own], [tuple(spot) for _, *spot in other], count
    )
    return pl.pallas_call(
        kernel,
        in_specs=[ANY] * count,
        out_specs=ANY,
        out_shape=jax.ShapeDtypeStruct((nvec, nvec), F32),
        input_output_aliases={len(blocks): 0} if earlier else {},
        scratch_shapes=[pltpu.SemaphoreType.DMA((24,))],
        compiler_params=pltpu.CompilerParams(vmem_limit_bytes=2**20),
    )(*blocks, *earlier)


def body(h_slab, vectors, left_rows):
    nvec = vectors.shape[1]
    wide = nvec // 8
    half = wide // 2
    opening, second, third, closing = products(h_slab.T, vectors)

    far, give, h_here = opening(2)
    other_far = shift(give, "core", 1)
    up, give, v_next = second(1, 3, h_here)
    other_up = shift(give, "core", 1)
    far = far + other_far
    from_below = shift(far[:half], "z", 1)
    from_above = shift(far[half:], "z", -1)
    down, give = third(h_here, v_next)
    other_down = shift(give, "core", 1)
    up, down = up + other_up, down + other_down
    up = jnp.concatenate([up[:half] + from_below, up[half:]])
    down = jnp.concatenate([down[:half], down[half:] + from_above])
    from_below = shift(up, "z", 1)
    from_above = shift(down, "z", -1)
    own, give = closing(0, h_here)
    shared = own + shift(give, "core", 1) + from_below + from_above

    local_part = lax.dot_general(
        left_rows.astype(F32),
        shared,
        (((0,), (1,)), ((), ())),
        precision=lax.Precision.HIGHEST,
        preferred_element_type=F32,
    )
    parts = local_part.reshape(16, nvec // 16, wide)
    parts = lax.all_to_all(parts, PLANE, 0, 0, tiled=True)
    summed = jnp.sum(parts, axis=0)
    copies = jnp.broadcast_to(summed, (16, *summed.shape))
    block = lax.all_to_all(
        copies, AXES, 0, 0, tiled=True, axis_index_groups=plane_groups()
    ).reshape(nvec, wide)

    low, high = block[: nvec // 2], block[nvec // 2 :]
    below_low = ring_shift(low, 1)
    above_high = ring_shift(high, -1)
    below_high = ring_shift(high, 1)
    above_low = ring_shift(low, -1)
    far_low = ring_shift(below_low, 1)
    far_high = ring_shift(above_high, -1)
    other = shift(block, "core", 1)
    other_below_low = shift(below_low, "core", 1)
    other_above_high = shift(above_high, "core", 1)
    other_below_high = shift(below_high, "core", 1)
    other_above_low = shift(above_low, "core", 1)
    whole = place([(block, 0, 0), (below_low, 3, 0), (above_high, 1, 1)], [(other, 0, 0)], None, nvec)
    other_far_low = shift(far_low, "core", 1)
    other_far_high = shift(far_high, "core", 1)
    own = [(below_high, 3, 1), (above_low, 1, 0)]
    others = [(other_below_low, 3, 0), (other_above_high, 1, 1), (other_below_high, 3, 1), (other_above_low, 1, 0)]
    whole = place(own, others, whole, nvec)
    return place([(far_low, 2, 0), (far_high, 2, 1)], [(other_far_low, 2, 0), (other_far_high, 2, 1)], whole, nvec)


def solution(mesh):
    fine = Mesh(mesh.devices.reshape(SIZES), AXES)
    row, col = ("y", "xh"), ("z", "xl", "core")
    in_specs = (P(row, col), P(col, None), P(row, None))
    return jax.shard_map(body, mesh=fine, in_specs=in_specs, out_specs=P(), check_vma=False)
```

```python
import functools

import jax
import jax.numpy as jnp
from jax import lax
from jax.experimental import pallas as pl
from jax.experimental.pallas import tpu as pltpu
from jax.sharding import Mesh, PartitionSpec as P


AXES = ("y", "xh", "z", "xl", "core")
SIZES = (4, 2, 4, 2, 2)
PLANE = ("y", "xh", "xl")
F32 = jnp.float32
ANY = pl.BlockSpec(memory_space=pl.ANY)
HBM = pl.BlockSpec(memory_space=pltpu.HBM)
VMEM = pl.BlockSpec(memory_space=pltpu.VMEM)


def rank(y, x, z, core):
    return (((y * 2 + x // 2) * 4 + z) * 2 + x % 2) * 2 + core


def shift(value, axis, step):
    size = lax.axis_size(axis)
    return lax.ppermute(value, axis, [(i, (i + step) % size) for i in range(size)])


def pair_up(value, turn):
    peer = [[1, 0, 3, 2], [3, 2, 1, 0]][turn]
    pairs = []
    for y in range(4):
        for x in range(4):
            for z in range(4):
                pairs.append((rank(y, x, z, 0), rank(y, x, peer[z], 0)))
                pairs.append((rank(y, x, z, 1), rank(peer[y], x, z, 1)))
    return lax.ppermute(value, AXES, pairs)


def found(here, step):
    if step in (1, 3):
        step = step + (2 - step) * 2 * lax.rem(here, 2)
    return lax.rem(here + step, 4)


def plane_groups():
    groups = [[rank(y, x, z, 0) for y in range(4) for x in range(4)] for z in range(4)]
    return groups + [[rank(y, x, z, 1) for z in range(4) for x in range(4)] for y in range(4)]


def resident(value):
    return pltpu.with_memory_space_constraint(value, pltpu.VMEM)


def streamed(value):
    return pltpu.with_memory_space_constraint(value, pltpu.HBM)


def cuts(depth):
    return [(start, min(1536, depth - start)) for start in range(0, depth, 1536)]


def multiply(left, right):
    return lax.dot_general(left, right, (((0,), (0,)), ((), ())), preferred_element_type=F32)


def columns_of(v, ahead, rows):
    width = v.shape[1] // 4
    column = pl.multiple_of(lax.rem(lax.axis_index("z") + ahead, 4) * width, width)
    return v.at[rows, pl.ds(column, width)]


def emit(total, keep, give):
    core = lax.axis_index("core")
    rows = total.shape[0] // 2
    keep[...] = total[pl.ds(pl.multiple_of(core * rows, rows), rows), :]
    give[...] = total[pl.ds(pl.multiple_of((1 - core) * rows, rows), rows), :]


def fetch(v, ahead, here, sem, base):
    copies = []
    for i, (start, size) in enumerate(cuts(v.shape[0])):
        rows = pl.ds(start, size)
        copies.append(pltpu.make_async_copy(columns_of(v, ahead, rows), here.at[rows], sem.at[base + i]))
    return copies


def accumulate(total, v_here, h_here, start, size):
    part = multiply(v_here[start : start + size], h_here[start : start + size])
    if start == 0:
        total[...] = part
    else:
        total[...] += part


def opening_kernel(ahead, h, v, keep, give, h_here, v_here, total, sem):
    spans = cuts(h.shape[0])
    ours = fetch(v, ahead, v_here, sem, 0)
    slab = []
    for i, (start, size) in enumerate(spans):
        rows = pl.ds(start, size)
        slab.append(pltpu.make_async_copy(h.at[rows], h_here.at[rows], sem.at[len(spans) + i]))
    for one, two in zip(slab, ours):
        one.start()
        two.start()
    for (start, size), one, two in zip(spans, slab, ours):
        one.wait()
        two.wait()
        accumulate(total, v_here, h_here, start, size)
    emit(total, keep, give)


def second_kernel(ahead, following, h_here, v, keep, give, v_next, v_here, total, sem):
    spans = cuts(v.shape[0])
    ours = fetch(v, ahead, v_here, sem, 0)
    theirs = fetch(v, following, v_next, sem, len(spans))
    for copy in (*ours, *theirs):
        copy.start()
    for (start, size), copy in zip(spans, ours):
        copy.wait()
        accumulate(total, v_here, h_here, start, size)
    emit(total, keep, give)
    for copy in theirs:
        copy.wait()


def third_kernel(following, h_here, v_here, v, keep, give, v_next, total, sem):
    theirs = fetch(v, following, v_next, sem, 0)
    for copy in theirs:
        copy.start()
    step = v.shape[0] // 3
    total[...] = jnp.zeros_like(total)

    @pl.loop(0, 3)
    def _(i):
        rows = pl.ds(pl.multiple_of(i * step, 16), step)
        total[...] += multiply(v_here[rows, :], h_here[rows, :])

    emit(total, keep, give)
    for copy in theirs:
        copy.wait()


def closing_kernel(h_here, v_here, keep, give, total):
    total[...] = multiply(v_here[...], h_here[...])
    emit(total, keep, give)


def kernel_call(kernel, h, v, ins, outs, scratch):
    width, rows = v.shape[1] // 4, h.shape[1]
    piece = pltpu.VMEM((width // 2, rows), F32)
    return pl.pallas_call(
        kernel,
        in_specs=ins,
        out_specs=[VMEM] * (2 + len(outs)),
        out_shape=[piece, piece, *outs],
        scratch_shapes=scratch,
        cost_estimate=pl.CostEstimate(flops=2 * h.shape[0] * width * rows, bytes_accessed=h.shape[0] * width * 2, transcendentals=0),
        compiler_params=pltpu.CompilerParams(vmem_limit_bytes=8 * 2**20),
    )


def products(h, v):
    depth, rows = h.shape
    block = pltpu.VMEM((depth, v.shape[1] // 4), v.dtype)
    slab = pltpu.VMEM((depth, rows), h.dtype)
    total = pltpu.VMEM((v.shape[1] // 4, rows), F32)
    v = streamed(v)
    sems = pltpu.SemaphoreType.DMA((2 * len(cuts(depth)),))

    def opening(ahead):
        kernel = functools.partial(opening_kernel, ahead)
        return kernel_call(kernel, h, v, [HBM, HBM], [slab], [block, total, sems])(streamed(h), v)

    def second(ahead, following, h_here):
        kernel = functools.partial(second_kernel, ahead, following)
        call = kernel_call(kernel, h, v, [VMEM, HBM], [block], [block, total, sems])
        return call(resident(h_here), v)

    def third(following, h_here, v_here):
        kernel = functools.partial(third_kernel, following)
        call = kernel_call(kernel, h, v, [VMEM, VMEM, HBM], [block], [total, sems])
        return call(resident(h_here), resident(v_here), v)

    def closing(h_here, v_here):
        call = kernel_call(closing_kernel, h, v, [VMEM, VMEM], [], [total])
        return call(resident(h_here), resident(v_here))

    return opening, second, third, closing


def near_kernel(*refs):
    own, other, out, sem = refs[:5], refs[5:10], refs[10], refs[11]
    spots = ((0, None), (1, 0), (1, 1), (3, 0), (3, 1))

    def spread(blocks):
        return [(ref, step, part) for ref, (step, part) in zip(blocks, spots)]

    write(spread(own), spread(other), out, sem)


def far_kernel(*refs):
    own, other, out, sem = refs[:2], refs[2:4], refs[5], refs[6]
    write([(own[0], 2, 0), (own[1], 2, 1)], [(other[0], 2, 0), (other[1], 2, 1)], out, sem)


def write(own, other, out, sem):
    y, z, core = lax.axis_index("y"), lax.axis_index("z"), lax.axis_index("core")

    def run(first, second):
        made = []
        for ref, step, part in first:
            rows, part = ref.shape[0], part or 0
            column = pl.multiple_of(found(z, step) * 256, 256)
            made.append((ref, out.at[pl.ds(part * rows, rows), pl.ds(column, 128)]))
        for ref, step, part in second:
            part = part or 0
            row = pl.multiple_of(found(y, step) * 256, 256)
            for k in range(ref.shape[0] // 256):
                column = (part * 2 + k) * 256 + 128
                made.append((ref.at[pl.ds(k * 256, 256)], out.at[pl.ds(row, 256), pl.ds(column, 128)]))
        made = [pltpu.make_async_copy(src, dst, sem.at[i]) for i, (src, dst) in enumerate(made)]
        for copy in made:
            copy.start()
        for copy in made:
            copy.wait()

    @pl.when(core == 0)
    def _():
        run(own, other)

    @pl.when(core == 1)
    def _():
        run(other, own)


def place_near(own, other, nvec):
    return pl.pallas_call(
        near_kernel,
        in_specs=[ANY] * 10,
        out_specs=ANY,
        out_shape=jax.ShapeDtypeStruct((nvec, nvec), F32),
        scratch_shapes=[pltpu.SemaphoreType.DMA((17,))],
        compiler_params=pltpu.CompilerParams(vmem_limit_bytes=2**20),
        name="place_near",
    )(*own, *other)


def place_far(own, other, whole):
    return pl.pallas_call(
        far_kernel,
        in_specs=[ANY] * 5,
        out_specs=ANY,
        out_shape=jax.ShapeDtypeStruct(whole.shape, F32),
        input_output_aliases={4: 0},
        scratch_shapes=[pltpu.SemaphoreType.DMA((6,))],
        compiler_params=pltpu.CompilerParams(vmem_limit_bytes=2**20),
        name="place_far",
    )(*own, *other, whole)


def body(h_slab, vectors, left_rows):
    nvec = vectors.shape[1]
    wide = nvec // 8
    half = wide // 2
    opening, second, third, closing = products(h_slab.T, vectors)

    far, give, h_here = opening(2)
    other_far = shift(give, "core", 1)
    up, give, v_next = second(1, 3, h_here)
    other_up = shift(give, "core", 1)
    far = far + other_far
    from_below = shift(far[:half], "z", 1)
    from_above = shift(far[half:], "z", -1)
    down, give, v_next = third(0, h_here, v_next)
    other_down = shift(give, "core", 1)
    up, down = up + other_up, down + other_down
    up = jnp.concatenate([up[:half] + from_below, up[half:]])
    down = jnp.concatenate([down[:half], down[half:] + from_above])
    from_below = shift(up, "z", 1)
    from_above = shift(down, "z", -1)
    own, give = closing(h_here, v_next)
    shared = own + shift(give, "core", 1) + from_below + from_above

    local_part = lax.dot_general(
        left_rows.astype(F32),
        shared,
        (((0,), (1,)), ((), ())),
        precision=lax.Precision.HIGHEST,
        preferred_element_type=F32,
    )
    parts = local_part.reshape(16, nvec // 16, wide)
    parts = lax.all_to_all(parts, PLANE, 0, 0, tiled=True)
    summed = jnp.sum(parts, axis=0)
    copies = jnp.broadcast_to(summed, (16, *summed.shape))
    block = lax.all_to_all(
        copies, AXES, 0, 0, tiled=True, axis_index_groups=plane_groups()
    ).reshape(nvec, wide)

    low, high = block[: nvec // 2], block[nvec // 2 :]
    one_low = pair_up(low, 0)
    two_high = pair_up(high, 1)
    one_high = pair_up(high, 0)
    two_low = pair_up(low, 1)
    far_low = pair_up(one_low, 1)
    far_high = pair_up(two_high, 0)
    other = shift(block, "core", 1)
    near = [one_low, one_high, two_low, two_high]
    other_near = [shift(value, "core", 1) for value in near]
    whole = place_near([block, *near], [other, *other_near], nvec)
    far = [far_low, far_high]
    return place_far(far, [shift(value, "core", 1) for value in far], whole)


def solution(mesh):
    fine = Mesh(mesh.devices.reshape(SIZES), AXES)
    row, col = ("y", "xh"), ("z", "xl", "core")
    in_specs = (P(row, col), P(col, None), P(row, None))
    return jax.shard_map(body, mesh=fine, in_specs=in_specs, out_specs=P(), check_vma=False)
```
